8 devices in a mesh: dp: 2 (over y, z), tp: 4 (over x, core).
Axes of the slice: x: 2, y: 2, z: 1, core: 2. Of those that a mesh axis runs over, the one named last changes fastest.
Arguments:
- x: bfloat16 [2048, 4096], P(('dp', 'tp')), parts along dimension 0
- gain: bfloat16 [4096], replicated
- wq: bfloat16 [4096, 6144], P(None, 'tp')
- wk: bfloat16 [4096, 1024], P(None, 'tp')
- wv: bfloat16 [4096, 1024], P(None, 'tp')
- wo: bfloat16 [6144, 4096], P('tp')
Outputs:
- output: bfloat16 [2048, 4096], P(('dp', 'tp')), parts along dimension 0
There are 2 independent parts. The reference program is written for one: setup_inputs(seed, part) draws one part's arguments, and reference() takes and returns one part's arrays. A program takes and returns all parts, laid end to end along the dimension named above; an argument that names none is the same for every part.
All inputs are finite; a program needn't handle non-finite values.
Results may differ from the reference program's by a relative error of at most 0.012.
Values are sent between devices in bfloat16 or wider.
A program may use at most 2 GiB of HBM per device.

```python
import jax
import jax.numpy as jnp
from jax import lax

ROWS = 1024
D = 4096
HEADS = 48
KV_HEADS = 8
HEAD = 128
THETA = 10000


def setup_inputs(seed: int = 0, part: int = 0) -> dict:
    kx, kn, kq, kk, kv, ko = jax.random.split(jax.random.key(seed), 6)

    def weights(key, rows, columns):
        return jax.random.normal(key, (rows, columns), jnp.float32) * rows**-0.5

    drawn = {
        "x": jax.random.normal(jax.random.fold_in(kx, part), (ROWS, D), jnp.float32),
        "gain": 1 + 0.1 * jax.random.normal(kn, (D,), jnp.float32),
        "wq": 2 * weights(kq, D, HEADS * HEAD),
        "wk": 2 * weights(kk, D, KV_HEADS * HEAD),
        "wv": 4 * weights(kv, D, KV_HEADS * HEAD),
        "wo": weights(ko, HEADS * HEAD, D),
    }
    return {k: v.astype(jnp.bfloat16) for k, v in drawn.items()}


def normed(x, gain):
    wide = x.astype(jnp.float32)
    scale = lax.rsqrt(jnp.mean(wide * wide, -1, keepdims=True) + 1e-6)
    return (wide * scale * gain.astype(jnp.float32)).astype(jnp.bfloat16)


def turned(t, place, theta):
    half = t.shape[-1] // 2
    angle = place.astype(jnp.float32)[:, None] * theta ** (-jnp.arange(half, dtype=jnp.float32) / half)
    cos, sin = jnp.cos(angle)[:, None], jnp.sin(angle)[:, None]
    a, b = t[..., :half].astype(jnp.float32), t[..., half:].astype(jnp.float32)
    return jnp.concatenate([a * cos - b * sin, b * cos + a * sin], -1).astype(jnp.bfloat16)


def matmul(a, w):
    return jnp.dot(a, w, preferred_element_type=jnp.float32).astype(jnp.bfloat16)


def einsum(form, a, b):
    return jnp.einsum(form, a.astype(jnp.float32), b.astype(jnp.float32))


def attention(q, k, v):
    scores = einsum("tgsd,ugd->gstu", q, k) * q.shape[-1] ** -0.5
    token = jnp.arange(q.shape[0])
    scores = jnp.where(token[:, None] >= token, scores, -jnp.inf)
    weights = jax.nn.softmax(scores, -1).astype(jnp.bfloat16)
    return einsum("gstu,ugd->tgsd", weights, v).astype(jnp.bfloat16)


def reference(x, gain, wq, wk, wv, wo):
    a, place = normed(x, gain), jnp.arange(ROWS)
    q = turned(matmul(a, wq).reshape(ROWS, HEADS, HEAD), place, THETA).reshape(ROWS, KV_HEADS, -1, HEAD)
    k = turned(matmul(a, wk).reshape(ROWS, KV_HEADS, HEAD), place, THETA)
    v = matmul(a, wv).reshape(ROWS, KV_HEADS, HEAD)
    seen = attention(q, k, v).reshape(ROWS, HEADS * HEAD)
    return (x.astype(jnp.float32) + jnp.dot(seen, wo, preferred_element_type=jnp.float32)).astype(jnp.bfloat16)
```

```python
import functools

import jax
import jax.numpy as jnp
import numpy as np
from jax import lax
from jax.experimental import pallas as pl
from jax.experimental.pallas import tpu as pltpu
from jax.sharding import PartitionSpec as P

HEAD = 128
THETA = 10000
NEG = -1e30
HIDDEN = 2 * NEG
LOG2E = 1.4426950408889634
TILE = 512
STRIP = 512
F32, BF16 = jnp.float32, jnp.bfloat16


def _dot(a, b, ca=1, cb=0):
    return lax.dot_general(a, b, (((ca,), (cb,)), ((), ())), preferred_element_type=F32)


def _layer(x_hbm, gain_hbm, tab_hbm, wq_hbm, wk_hbm, wv_hbm, wo_hbm, y_hbm,
           wq, wkv, wo, xs, a, gain, tab, rope, q, k, vt, top, mix, gap, seen, pp_out, pp_in, rs_out, rs_in, fin_in,
           ld, wo_ld, own_s, own_r, ag_s, ag_r, rl_s, rl_r, pp_s, pp_r, rs_s, rs_r, fin_s, fin_r, out_s):
    me = lax.axis_index("tp")
    chip, core = me // 2, me % 2
    mate, peer = chip * 2 + 1 - core, (me + 2) % 4
    base, far = chip * 2, 2 - chip * 2
    rows = a.shape[0]
    d = a.shape[1]
    nq, no = wq.shape[0], wo.shape[0]
    heads, kv = q.shape[1], k.shape[1]
    group = heads // kv
    per = STRIP // rows
    half = no // 2

    def stage(n):
        return wq.at[0, pl.ds(pl.multiple_of(n * rows, rows), rows)]

    def fin_out(n):
        return wq.at[1, pl.ds(pl.multiple_of(n * rows, rows), rows)]

    def send(src, dst, s, r, to):
        return pltpu.make_async_remote_copy(src, dst, s, r, device_id={"tp": to}, device_id_type=pl.DeviceIdType.MESH)

    def local_x(n):
        h = core if n == 0 else 1 - core
        return pltpu.make_async_copy(x_hbm.at[pl.ds(2 * h, 2)], xs.at[me, pl.ds(2 * h, 2)], ld.at[n])

    def own(n):
        h = 1 - core if n == 0 else core
        return send(x_hbm.at[pl.ds(2 * h, 2)], xs.at[me, pl.ds(2 * h, 2)], own_s.at[n], own_r.at[n], mate)

    def gather(m):
        at = xs.at[base + m // 2, 2 * core + m % 2]
        return send(at, at, ag_s.at[m], ag_r.at[m], peer)

    def relay(m):
        at = xs.at[far + m // 2, 2 * core + m % 2]
        return send(at, at, rl_s.at[m], rl_r.at[m], mate)

    def weights_q(n):
        return pltpu.make_async_copy(wq_hbm.at[:, pl.ds(pl.multiple_of(n * TILE, TILE), TILE)], wq.at[n], ld.at[6 + n])

    def weights_o(n):
        return pltpu.make_async_copy(wo_hbm.at[:, pl.ds(pl.multiple_of(n * TILE, TILE), TILE)], wo.at[n], wo_ld.at[n])

    wide = kv * HEAD
    small = [
        pltpu.make_async_copy(gain_hbm, gain, ld.at[2]),
        pltpu.make_async_copy(tab_hbm, tab, ld.at[3]),
        pltpu.make_async_copy(wk_hbm, wkv.at[:, pl.ds(0, wide)], ld.at[4]),
        pltpu.make_async_copy(wv_hbm, wkv.at[:, pl.ds(wide, wide)], ld.at[5]),
    ]

    def norm(blk):
        step = 32
        parts = xs.shape[2] // step

        def some(i, _):
            at = (blk, i // parts, pl.ds(pl.multiple_of((i % parts) * step, step), step))
            total = jnp.zeros((step, 128), F32)
            for c in range(0, d, 128):
                w = xs[(*at, pl.ds(c, 128))].astype(F32)
                total = total + w * w
            scale = lax.rsqrt(jnp.sum(total, axis=1, keepdims=True) * (1 / d) + 1e-6)
            for c in range(0, d, 128):
                w = xs[(*at, pl.ds(c, 128))].astype(F32)
                a[pl.ds(pl.multiple_of(i * step, step), step), pl.ds(c, 128)] = (w * scale * gain[:, pl.ds(c, 128)].astype(F32)).astype(BF16)
            return 0

        lax.fori_loop(0, rows // step, some, 0)

    def turned(t):
        t = t.astype(BF16).astype(F32)
        return (t * rope[0] + pltpu.roll(t, HEAD // 2, 1) * rope[1]).astype(BF16)

    def project(blk, loading):
        t = tab[pl.ds(pl.multiple_of(blk * rows, rows), rows), :]
        r = pltpu.roll(t, HEAD // 2, 1)
        first = lax.broadcasted_iota(jnp.int32, t.shape, 1) < HEAD // 2
        rope[0] = jnp.where(first, t, r)
        rope[1] = jnp.where(first, -r, t)
        if loading:
            small[2].wait()
            small[3].wait()
        got = _dot(a[...], wkv[...])
        for i in range(kv):
            k[blk, i] = turned(got[:, i * HEAD : (i + 1) * HEAD])
            vt[blk, i, :HEAD, :] = got[:, wide + i * HEAD : wide + (i + 1) * HEAD].T.astype(BF16)

        def some(n, _):
            if loading:
                weights_q(n).wait()
            got = _dot(a[...], wq[n])
            for i in range(TILE // HEAD):
                q[blk, n * (TILE // HEAD) + i] = turned(got[:, i * HEAD : (i + 1) * HEAD])
            return 0

        lax.fori_loop(0, nq, some, 0)

    def attend(blk):
        e = HEAD**-0.5 * LOG2E
        pieces = [(i, i * group + n) for i in range(kv) for n in range(0, group, per)]
        top[...] = jnp.full(top.shape, NEG, F32)
        mix[...] = jnp.zeros(mix.shape, F32)

        def block(j, masked):
            scores = [_dot(k[j, i], q[blk, pl.ds(n, per)].reshape(STRIP, HEAD), 1, 1) for i, n in pieces]
            weights, keeps = [], []
            for p, s in enumerate(scores):
                if masked:
                    s = jnp.where(gap[...] >= 0, s, HIDDEN)
                old = top[p : p + 1, :]
                new = jnp.maximum(old, s.max(axis=0, keepdims=True))
                top[p : p + 1, :] = new
                weights.append(jnp.exp2((s - new) * e).astype(BF16))
                keeps.append(jnp.exp2((old - new) * e))
            for p, (w, keep) in enumerate(zip(weights, keeps)):
                mix[p] = mix[p] * keep + _dot(vt[j, pieces[p][0]], w)

        lax.fori_loop(0, blk, lambda j, _: (block(j, False), 0)[1], 0)
        block(blk, True)
        for p, (i, n) in enumerate(pieces):
            got = mix[p, :HEAD, :] * (1 / mix[p, HEAD : HEAD + 1, :])
            for m in range(per):
                seen[:, (n + m) * HEAD : (n + m + 1) * HEAD] = got[:, m * rows : (m + 1) * rows].T.astype(BF16)

    def out_part(n):
        return _dot(seen[...], wo[n])

    def pass_on(b, t):
        return send(pp_out.at[t], pp_in.at[b * half + t], pp_s.at[t], pp_r.at[b * half + t], mate)

    def scatter(b, t):
        return send(rs_out.at[b * half + t], rs_in.at[core * half + t], rs_s.at[b * half + t], rs_r.at[core * half + t], far + b)

    def give(b):
        def mates(t, _):
            if b:
                pass_on(0, t).wait_send()
            pp_out[t] = out_part((1 - core) * half + t).astype(BF16)
            pass_on(b, t).start()
            return 0

        def mine(t, _):
            got = out_part(core * half + t)
            pass_on(b, t).wait_recv()
            rs_out[b * half + t] = (got + pp_in[b * half + t].astype(F32)).astype(BF16)
            scatter(b, t).start()
            return 0

        lax.fori_loop(0, half, mates, 0)
        lax.fori_loop(0, half, mine, 0)

    def last(n):
        return send(fin_out(n), fin_in.at[n], fin_s.at[n], fin_r.at[n], mate)

    def place(i):
        return (i % 2) * half + i // 2

    def mates_rows(i, _):
        n = place(i)
        fin_out(n)[...] = out_part(n).astype(BF16)
        last(n).start()
        return 0

    def store(n):
        return pltpu.make_async_copy(stage(n), y_hbm.at[:, pl.ds(pl.multiple_of(n * TILE, TILE), TILE)], out_s.at[n])

    def my_rows(i, _):
        n = place(i)
        got = out_part(n)
        last(n).wait_recv()
        send(rs_out.at[0], rs_in.at[n], rs_s.at[0], rs_r.at[n], peer).wait_recv()
        mine = xs[me, :, :, pl.ds(pl.multiple_of(n * TILE, TILE), TILE)].reshape(rows, TILE).astype(F32)
        stage(n)[...] = (mine + (got + fin_in[n].astype(F32) + rs_in[n].astype(F32))).astype(BF16)
        store(n).start()
        return 0

    local_x(0).start()
    local_x(1).start()
    for copy in small:
        copy.start()
    for n in range(nq):
        weights_q(n).start()
    barrier = pltpu.get_barrier_semaphore()
    for to in (mate, peer, (mate + 2) % 4):
        pl.semaphore_signal(barrier, 1, device_id={"tp": to}, device_id_type=pl.DeviceIdType.MESH)
    pl.semaphore_wait(barrier, 3)
    own(0).start()
    own(1).start()
    local_x(0).wait()

    @pl.when(core == 0)
    def _():
        gather(0).start()
        gather(1).start()

    own(0).wait_recv()

    @pl.when(core == 1)
    def _():
        gather(0).start()
        gather(1).start()

    gather(2).start()
    gather(3).start()

    gap[...] = lax.rem(lax.broadcasted_iota(jnp.int32, gap.shape, 1), rows) - lax.broadcasted_iota(jnp.int32, gap.shape, 0)
    vt[:, :, HEAD:, :] = jnp.ones((4, kv, vt.shape[2] - HEAD, rows), BF16)

    local_x(1).wait()
    small[0].wait()
    norm(me)
    small[1].wait()
    project(me, True)
    for n in range(no):
        weights_o(n).start()
    own(1).wait_recv()
    norm(mate)
    project(mate, False)

    for b in range(2):
        for m in (2 * b, 2 * b + 1):
            if m != 2:
                gather(m).wait_recv()
                relay(m).start()
        for m in (2 * b, 2 * b + 1):
            relay(m).wait_recv()
        norm(far + b)
        project(far + b, False)
        attend(far + b)
        if b == 0:
            gather(2).wait_recv()
            relay(2).start()
            for n in range(no):
                weights_o(n).wait()
        give(b)

    attend(mate)
    lax.fori_loop(0, no, mates_rows, 0)
    attend(me)
    lax.fori_loop(0, no, my_rows, 0)

    for n in range(2):
        own(n).wait_send()
    for m in range(4):
        gather(m).wait_send()
        relay(m).wait_send()
    for t in range(half):
        pass_on(1, t).wait_send()
    for n in range(no):
        scatter(n // half, n % half).wait_send()
        last(n).wait_send()
        store(n).wait()


def _table(tokens):
    half = HEAD // 2
    angle = np.arange(tokens, dtype=np.float32)[:, None] * np.float32(THETA) ** (-np.arange(half, dtype=np.float32) / np.float32(half))
    angle = angle.astype(np.float64)
    return np.concatenate([np.cos(angle), np.sin(angle)], -1).astype(np.float32)


def solution(mesh):
    def step(x, gain, wq, wk, wv, wo):
        rows, d = x.shape
        heads, kv = wq.shape[1] // HEAD, wk.shape[1] // HEAD
        nq, no = wq.shape[1] // TILE, d // TILE
        strips = heads * rows // STRIP
        dma = lambda n: pltpu.SemaphoreType.DMA((n,))
        vm = pltpu.VMEM
        tokens = 4 * rows
        return pl.pallas_call(
            _layer,
            out_shape=jax.ShapeDtypeStruct((rows, d), BF16),
            in_specs=[pl.BlockSpec(memory_space=pl.ANY)] * 7,
            out_specs=pl.BlockSpec(memory_space=pl.ANY),
            scratch_shapes=[
                vm((nq, d, TILE), BF16), vm((d, 2 * kv * HEAD), BF16), vm((no, heads * HEAD, TILE), BF16),
                vm((4, 4, rows // 4, d), BF16), vm((rows, d), BF16), vm((1, d), BF16), vm((tokens, HEAD), F32), vm((2, rows, HEAD), F32),
                vm((4, heads, rows, HEAD), BF16), vm((4, kv, rows, HEAD), BF16), vm((4, kv, HEAD + 16, rows), BF16),
                vm((strips, STRIP), F32), vm((strips, HEAD + 16, STRIP), F32), vm((rows, STRIP), jnp.int32), vm((rows, heads * HEAD), BF16),
                vm((no // 2, rows, TILE), BF16), vm((no, rows, TILE), BF16), vm((no, rows, TILE), BF16), vm((no, rows, TILE), BF16),
                vm((no, rows, TILE), BF16),
                dma(6 + nq), dma(no), dma(2), dma(2), dma(4), dma(4), dma(4), dma(4), dma(no // 2), dma(no), dma(no), dma(no),
                dma(no), dma(no), dma(no),
            ],
            compiler_params=pltpu.CompilerParams(collective_id=0, has_side_effects=True, vmem_limit_bytes=67043328),
            cost_estimate=pl.CostEstimate(flops=33 * 10**9, bytes_accessed=34 * 2**20, transcendentals=8 * 2**20),
            name="layer",
        )(x.reshape(4, rows // 4, d), gain.reshape(1, d), jnp.asarray(_table(tokens)), wq, wk, wv, wo)

    tokens, columns = P(("dp", "tp"), None), P(None, "tp")
    return jax.shard_map(
        step,
        mesh=mesh,
        in_specs=(tokens, P(None), columns, columns, columns, P("tp", None)),
        out_specs=tokens,
        check_vma=False,
    )
```

```python
import functools

import jax
import jax.numpy as jnp
import numpy as np
from jax import lax
from jax.experimental import pallas as pl
from jax.experimental.pallas import tpu as pltpu
from jax.sharding import PartitionSpec as P

HEAD = 128
THETA = 10000
NEG = -1e30
HIDDEN = 2 * NEG
LOG2E = 1.4426950408889634
TILE = 512
STRIP = 512
F32, BF16 = jnp.float32, jnp.bfloat16


def _dot(a, b, ca=1, cb=0):
    return lax.dot_general(a, b, (((ca,), (cb,)), ((), ())), preferred_element_type=F32)


def _layer(x_hbm, gain_hbm, tab_hbm, wq_hbm, wk_hbm, wv_hbm, wo_hbm, y,
           wq, wkv, wo, xs, a, gain, gain_w, tab, rope, q, k, vt, top, mix, gap, seen, pp_out, pp_in, rs_out, rs_in, fin_in,
           ld, wo_ld, own_s, own_r, ag_s, ag_r, rl_s, rl_r, pp_s, pp_r, rs_s, rs_r, fin_s, fin_r):
    me = lax.axis_index("tp")
    chip, core = me // 2, me % 2
    mate, peer = chip * 2 + 1 - core, (me + 2) % 4
    base, far = chip * 2, 2 - chip * 2
    rows = a.shape[0]
    d = a.shape[1]
    nq, no = wq.shape[0], wo.shape[0]
    heads, kv = q.shape[1], k.shape[1]
    group = heads // kv
    per = STRIP // rows
    half = no // 2

    def fin_out(n):
        return wq.at[1, pl.ds(pl.multiple_of(n * rows, rows), rows)]

    def send(src, dst, s, r, to):
        return pltpu.make_async_remote_copy(src, dst, s, r, device_id={"tp": to}, device_id_type=pl.DeviceIdType.MESH)

    def local_x(n):
        h = core if n == 0 else 1 - core
        return pltpu.make_async_copy(x_hbm.at[pl.ds(2 * h, 2)], xs.at[me, pl.ds(2 * h, 2)], ld.at[n])

    def own(n):
        h = 1 - core if n == 0 else core
        return send(x_hbm.at[pl.ds(2 * h, 2)], xs.at[me, pl.ds(2 * h, 2)], own_s.at[n], own_r.at[n], mate)

    def gather(m):
        at = xs.at[base + m // 2, 2 * core + m % 2]
        return send(at, at, ag_s.at[m], ag_r.at[m], peer)

    def relay(m):
        at = xs.at[far + m // 2, 2 * core + m % 2]
        return send(at, at, rl_s.at[m], rl_r.at[m], mate)

    def weights_q(n):
        return pltpu.make_async_copy(wq_hbm.at[:, pl.ds(pl.multiple_of(n * TILE, TILE), TILE)], wq.at[n], ld.at[6 + n])

    def weights_o(n):
        return pltpu.make_async_copy(wo_hbm.at[:, pl.ds(pl.multiple_of(n * TILE, TILE), TILE)], wo.at[n], wo_ld.at[n])

    wide = kv * HEAD
    small = [
        pltpu.make_async_copy(gain_hbm, gain, ld.at[2]),
        pltpu.make_async_copy(tab_hbm, tab, ld.at[3]),
        pltpu.make_async_copy(wk_hbm, wkv.at[:, pl.ds(0, wide)], ld.at[4]),
        pltpu.make_async_copy(wv_hbm, wkv.at[:, pl.ds(wide, wide)], ld.at[5]),
    ]

    def norm(blk):
        step = 32
        parts = xs.shape[2] // step

        def some(i, _):
            at = (blk, i // parts, pl.ds(pl.multiple_of((i % parts) * step, step), step))
            total = jnp.zeros((step, 128), F32)
            for c in range(0, d, 128):
                w = xs[(*at, pl.ds(c, 128))].astype(F32)
                total = total + w * w
            scale = lax.rsqrt(jnp.sum(total, axis=1, keepdims=True) * (1 / d) + 1e-6)
            for c in range(0, d, 128):
                w = xs[(*at, pl.ds(c, 128))].astype(F32)
                a[pl.ds(pl.multiple_of(i * step, step), step), pl.ds(c, 128)] = (w * scale * gain_w[pl.ds(c // 128, 1), :]).astype(BF16)
            return 0

        lax.fori_loop(0, rows // step, some, 0)

    def turned(t):
        t = t.astype(BF16).astype(F32)
        return (t * rope[0] + pltpu.roll(t, HEAD // 2, 1) * rope[1]).astype(BF16)

    def project(blk, loading):
        t = tab[pl.ds(pl.multiple_of(blk * rows, rows), rows), :]
        r = pltpu.roll(t, HEAD // 2, 1)
        first = lax.broadcasted_iota(jnp.int32, t.shape, 1) < HEAD // 2
        rope[0] = jnp.where(first, t, r)
        rope[1] = jnp.where(first, -r, t)
        if loading:
            small[2].wait()
            small[3].wait()
        got = _dot(a[...], wkv[...])
        for i in range(kv):
            k[blk, i] = turned(got[:, i * HEAD : (i + 1) * HEAD])
            vt[blk, i, :HEAD, :] = got[:, wide + i * HEAD : wide + (i + 1) * HEAD].T.astype(BF16)

        def some(n, _):
            if loading:
                weights_q(n).wait()
            got = _dot(a[...], wq[n])
            for i in range(TILE // HEAD):
                q[blk, n * (TILE // HEAD) + i] = turned(got[:, i * HEAD : (i + 1) * HEAD])
            return 0

        lax.fori_loop(0, nq, some, 0)

    def attend(blk):
        e = HEAD**-0.5 * LOG2E
        pieces = [(i, i * group + n) for i in range(kv) for n in range(0, group, per)]
        top[...] = jnp.full(top.shape, NEG, F32)
        mix[...] = jnp.zeros(mix.shape, F32)

        def block(j, masked):
            scores = [_dot(k[j, i], q[blk, pl.ds(n, per)].reshape(STRIP, HEAD), 1, 1) for i, n in pieces]
            weights, keeps = [], []
            for p, s in enumerate(scores):
                if masked:
                    s = jnp.where(gap[...] >= 0, s, HIDDEN)
                old = top[p : p + 1, :]
                new = jnp.maximum(old, s.max(axis=0, keepdims=True))
                top[p : p + 1, :] = new
                weights.append(jnp.exp2((s - new) * e).astype(BF16))
                keeps.append(jnp.exp2((old - new) * e))
            for p, (w, keep) in enumerate(zip(weights, keeps)):
                mix[p] = mix[p] * keep + _dot(vt[j, pieces[p][0]], w)

        lax.fori_loop(0, blk, lambda j, _: (block(j, False), 0)[1], 0)
        block(blk, True)
        for p, (i, n) in enumerate(pieces):
            got = mix[p, :HEAD, :] * (1 / mix[p, HEAD : HEAD + 1, :])
            for m in range(per):
                seen[:, (n + m) * HEAD : (n + m + 1) * HEAD] = got[:, m * rows : (m + 1) * rows].T.astype(BF16)

    def out_part(n):
        return _dot(seen[...], wo[n])

    def pass_on(b, t):
        return send(pp_out.at[t], pp_in.at[b * half + t], pp_s.at[t], pp_r.at[b * half + t], mate)

    def scatter(b, t):
        return send(rs_out.at[b * half + t], rs_in.at[core * half + t], rs_s.at[b * half + t], rs_r.at[core * half + t], far + b)

    def give(b):
        def mates(t, _):
            if b:
                pass_on(0, t).wait_send()
            pp_out[t] = out_part((1 - core) * half + t).astype(BF16)
            pass_on(b, t).start()
            return 0

        def mine(t, _):
            got = out_part(core * half + t)
            pass_on(b, t).wait_recv()
            rs_out[b * half + t] = (got + pp_in[b * half + t].astype(F32)).astype(BF16)
            scatter(b, t).start()
            return 0

        lax.fori_loop(0, half, mates, 0)
        lax.fori_loop(0, half, mine, 0)

    def last(n):
        return send(fin_out(n), fin_in.at[n], fin_s.at[n], fin_r.at[n], mate)

    def place(i):
        return (i % 2) * half + i // 2

    def mates_rows(i, _):
        n = place(i)
        fin_out(n)[...] = out_part(n).astype(BF16)
        last(n).start()
        return 0

    def my_rows(i, _):
        n = place(i)
        got = out_part(n)
        last(n).wait_recv()
        send(rs_out.at[0], rs_in.at[n], rs_s.at[0], rs_r.at[n], peer).wait_recv()
        mine = xs[me, :, :, pl.ds(pl.multiple_of(n * TILE, TILE), TILE)].reshape(rows, TILE).astype(F32)
        y[:, pl.ds(pl.multiple_of(n * TILE, TILE), TILE)] = (mine + (got + fin_in[n].astype(F32) + rs_in[n].astype(F32))).astype(BF16)
        return 0

    local_x(0).start()
    local_x(1).start()
    for copy in small:
        copy.start()
    for n in range(nq):
        weights_q(n).start()
    barrier = pltpu.get_barrier_semaphore()
    for to in (mate, peer, (mate + 2) % 4):
        pl.semaphore_signal(barrier, 1, device_id={"tp": to}, device_id_type=pl.DeviceIdType.MESH)
    pl.semaphore_wait(barrier, 3)
    own(0).start()
    own(1).start()
    local_x(0).wait()

    @pl.when(core == 0)
    def _():
        gather(0).start()
        gather(1).start()

    own(0).wait_recv()

    @pl.when(core == 1)
    def _():
        gather(0).start()
        gather(1).start()

    gather(2).start()
    gather(3).start()

    gap[...] = lax.rem(lax.broadcasted_iota(jnp.int32, gap.shape, 1), rows) - lax.broadcasted_iota(jnp.int32, gap.shape, 0)
    vt[:, :, HEAD:, :] = jnp.ones((4, kv, vt.shape[2] - HEAD, rows), BF16)

    local_x(1).wait()
    small[0].wait()
    gain_w[...] = gain[...].astype(F32)
    norm(me)
    small[1].wait()
    project(me, True)
    for n in range(no):
        weights_o(n).start()
    own(1).wait_recv()
    norm(mate)
    project(mate, False)

    for b in range(2):
        for m in (2 * b, 2 * b + 1):
            if m != 2:
                gather(m).wait_recv()
                relay(m).start()
        for m in (2 * b, 2 * b + 1):
            relay(m).wait_recv()
        norm(far + b)
        project(far + b, False)
        attend(far + b)
        if b == 0:
            gather(2).wait_recv()
            relay(2).start()
            for n in range(no):
                weights_o(n).wait()
        give(b)

    attend(mate)
    lax.fori_loop(0, no, mates_rows, 0)
    attend(me)
    lax.fori_loop(0, no, my_rows, 0)

    for n in range(2):
        own(n).wait_send()
    for m in range(4):
        gather(m).wait_send()
        relay(m).wait_send()
    for t in range(half):
        pass_on(1, t).wait_send()
    for n in range(no):
        scatter(n // half, n % half).wait_send()
        last(n).wait_send()


def _table(tokens):
    half = HEAD // 2
    angle = np.arange(tokens, dtype=np.float32)[:, None] * np.float32(THETA) ** (-np.arange(half, dtype=np.float32) / np.float32(half))
    angle = angle.astype(np.float64)
    return np.concatenate([np.cos(angle), np.sin(angle)], -1).astype(np.float32)


def solution(mesh):
    def step(x, gain, wq, wk, wv, wo):
        rows, d = x.shape
        heads, kv = wq.shape[1] // HEAD, wk.shape[1] // HEAD
        nq, no = wq.shape[1] // TILE, d // TILE
        strips = heads * rows // STRIP
        dma = lambda n: pltpu.SemaphoreType.DMA((n,))
        vm = pltpu.VMEM
        tokens = 4 * rows
        return pl.pallas_call(
            _layer,
            out_shape=pltpu.VMEM((rows, d), BF16),
            in_specs=[pl.BlockSpec(memory_space=pl.ANY)] * 7,
            out_specs=pl.BlockSpec(memory_space=pltpu.VMEM),
            scratch_shapes=[
                vm((nq, d, TILE), BF16), vm((d, 2 * kv * HEAD), BF16), vm((no, heads * HEAD, TILE), BF16),
                vm((4, 4, rows // 4, d), BF16), vm((rows, d), BF16), vm((d // 128, 128), BF16), vm((d // 128, 128), F32), vm((tokens, HEAD), F32), vm((2, rows, HEAD), F32),
                vm((4, heads, rows, HEAD), BF16), vm((4, kv, rows, HEAD), BF16), vm((4, kv, HEAD + 16, rows), BF16),
                vm((strips, STRIP), F32), vm((strips, HEAD + 16, STRIP), F32), vm((rows, STRIP), jnp.int32), vm((rows, heads * HEAD), BF16),
                vm((no // 2, rows, TILE), BF16), vm((no, rows, TILE), BF16), vm((no, rows, TILE), BF16), vm((no, rows, TILE), BF16),
                vm((no, rows, TILE), BF16),
                dma(6 + nq), dma(no), dma(2), dma(2), dma(4), dma(4), dma(4), dma(4), dma(no // 2), dma(no), dma(no), dma(no),
                dma(no), dma(no),
            ],
            compiler_params=pltpu.CompilerParams(collective_id=0, has_side_effects=True, vmem_limit_bytes=247 * 2**18),
            cost_estimate=pl.CostEstimate(flops=33 * 10**9, bytes_accessed=34 * 2**20, transcendentals=8 * 2**20),
            name="layer",
        )(x.reshape(4, rows // 4, d), gain.reshape(d // 128, 128), jnp.asarray(_table(tokens)), wq, wk, wv, wo)

    tokens, columns = P(("dp", "tp"), None), P(None, "tp")
    return jax.shard_map(
        step,
        mesh=mesh,
        in_specs=(tokens, P(None), columns, columns, columns, P("tp", None)),
        out_specs=tokens,
        check_vma=False,
    )
```

```python
import functools

import jax
import jax.numpy as jnp
import numpy as np
from jax import lax
from jax.experimental import pallas as pl
from jax.experimental.pallas import tpu as pltpu
from jax.sharding import PartitionSpec as P

HEAD = 128
THETA = 10000
NEG = -1e30
HIDDEN = 2 * NEG
LOG2E = 1.4426950408889634
TILE = 512
STRIP = 512
F32, BF16 = jnp.float32, jnp.bfloat16


def _dot(a, b, ca=1, cb=0):
    return lax.dot_general(a, b, (((ca,), (cb,)), ((), ())), preferred_element_type=F32)


def _layer(x_hbm, gain_hbm, tab_hbm, wq_hbm, wk_hbm, wv_hbm, wo_hbm, y,
           wq, wkv, wo, xs, a, gain, gain_w, tab, rope, q, k, vt, top, mix, gap, seen, pp_out, pp_in, rs_out, rs_in, fin_in,
           ld, wo_ld, own_s, own_r, ag_s, ag_r, rl_s, rl_r, pp_s, pp_r, rs_s, rs_r, fin_s, fin_r):
    me = lax.axis_index("tp")
    chip, core = me // 2, me % 2
    mate, peer = chip * 2 + 1 - core, (me + 2) % 4
    base, far = chip * 2, 2 - chip * 2
    rows = a.shape[0]
    d = a.shape[1]
    nq, no = wq.shape[0], wo.shape[0]
    heads, kv = q.shape[1], k.shape[1]
    group = heads // kv
    per = STRIP // rows
    half = no // 2
    hu = xs.shape[1] // 2

    def fin_out(n):
        return wq.at[1, pl.ds(pl.multiple_of(n * rows, rows), rows)]

    def send(src, dst, s, r, to):
        return pltpu.make_async_remote_copy(src, dst, s, r, device_id={"tp": to}, device_id_type=pl.DeviceIdType.MESH)

    def local_x(n):
        h = core if n < 2 else 1 - core
        at = pl.ds(h * hu + (n == 1), (1, hu - 1, hu)[n])
        return pltpu.make_async_copy(x_hbm.at[at], xs.at[me, at], ld.at[n])

    def own(n):
        at = pl.ds((1 - core if n == 0 else core) * hu, hu)
        return send(x_hbm.at[at], xs.at[me, at], own_s.at[n], own_r.at[n], mate)

    def message(m, first):
        blk, at, n = ((0, 0, 1), (0, 1, hu // 2 - 1), (0, hu // 2, hu // 2), (1, 0, hu // 2), (1, hu // 2, hu // 2))[m]
        return xs.at[first + blk, pl.ds(core * hu + at, n)]

    def gather(m):
        at = message(m, base)
        return send(at, at, ag_s.at[m], ag_r.at[m], peer)

    def relay(m):
        at = message(m, far)
        return send(at, at, rl_s.at[m], rl_r.at[m], mate)

    def weights_q(n):
        return pltpu.make_async_copy(wq_hbm.at[:, pl.ds(pl.multiple_of(n * TILE, TILE), TILE)], wq.at[n], ld.at[7 + n])

    def weights_o(n):
        return pltpu.make_async_copy(wo_hbm.at[:, pl.ds(pl.multiple_of(n * TILE, TILE), TILE)], wo.at[n], wo_ld.at[n])

    wide = kv * HEAD
    small = [
        pltpu.make_async_copy(gain_hbm, gain, ld.at[3]),
        pltpu.make_async_copy(tab_hbm, tab, ld.at[4]),
        pltpu.make_async_copy(wk_hbm, wkv.at[:, pl.ds(0, wide)], ld.at[5]),
        pltpu.make_async_copy(wv_hbm, wkv.at[:, pl.ds(wide, wide)], ld.at[6]),
    ]

    def norm(blk):
        step = 32
        units = step // xs.shape[2]

        def some(i, _):
            at = (blk, pl.ds(i * units, units))
            total = jnp.zeros((step, 128), F32)
            for c in range(0, d, 128):
                w = xs[(*at, slice(None), pl.ds(c, 128))].reshape(step, 128).astype(F32)
                total = total + w * w
            scale = lax.rsqrt(jnp.sum(total, axis=1, keepdims=True) * (1 / d) + 1e-6)
            for c in range(0, d, 128):
                w = xs[(*at, slice(None), pl.ds(c, 128))].reshape(step, 128).astype(F32)
                a[pl.ds(pl.multiple_of(i * step, step), step), pl.ds(c, 128)] = (w * scale * gain_w[pl.ds(c // 128, 1), :]).astype(BF16)
            return 0

        lax.fori_loop(0, rows // step, some, 0)

    def turned(t):
        t = t.astype(BF16).astype(F32)
        return (t * rope[0] + pltpu.roll(t, HEAD // 2, 1) * rope[1]).astype(BF16)

    def project(blk, loading):
        t = tab[pl.ds(pl.multiple_of(blk * rows, rows), rows), :]
        r = pltpu.roll(t, HEAD // 2, 1)
        first = lax.broadcasted_iota(jnp.int32, t.shape, 1) < HEAD // 2
        rope[0] = jnp.where(first, t, r)
        rope[1] = jnp.where(first, -r, t)
        if loading:
            small[2].wait()
            small[3].wait()
        got = _dot(a[...], wkv[...])
        for i in range(kv):
            k[blk, i] = turned(got[:, i * HEAD : (i + 1) * HEAD])
            vt[blk, i, :HEAD, :] = got[:, wide + i * HEAD : wide + (i + 1) * HEAD].T.astype(BF16)

        def some(n, _):
            if loading:
                weights_q(n).wait()
            got = _dot(a[...], wq[n])
            for i in range(TILE // HEAD):
                q[blk, n * (TILE // HEAD) + i] = turned(got[:, i * HEAD : (i + 1) * HEAD])
            return 0

        lax.fori_loop(0, nq, some, 0)

    def attend(blk):
        e = HEAD**-0.5 * LOG2E
        deep = vt.shape[2]
        pieces = [(i, i * group + n) for i in range(kv) for n in range(0, group, per)]
        top[...] = jnp.full(top.shape, NEG, F32)
        mix[...] = jnp.zeros(mix.shape, F32)

        def block(j, masked):
            scores = [_dot(k[j, i], q[blk, pl.ds(n, per)].reshape(STRIP, HEAD), 1, 1) for i, n in pieces]
            weights, keeps = [], []
            for p, s in enumerate(scores):
                if masked:
                    s = jnp.where(gap[...] >= 0, s, HIDDEN)
                old = top[p : p + 1, :]
                new = jnp.maximum(old, s.max(axis=0, keepdims=True))
                top[p : p + 1, :] = new
                weights.append(jnp.exp2((s - new) * e).astype(BF16))
                keeps.append(jnp.exp2((old - new) * e))
            for p, (w, keep) in enumerate(zip(weights, keeps)):
                at = pl.ds(p * deep, deep)
                mix[at, :] = mix[at, :] * keep + _dot(vt[j, pieces[p][0]], w)

        lax.fori_loop(0, blk, lambda j, _: (block(j, False), 0)[1], 0)
        block(blk, True)
        for p, (i, n) in enumerate(pieces):
            got = mix[p * deep : p * deep + HEAD, :] * (1 / mix[p * deep + HEAD : p * deep + HEAD + 1, :])
            for m in range(per):
                seen[:, (n + m) * HEAD : (n + m + 1) * HEAD] = got[:, m * rows : (m + 1) * rows].T.astype(BF16)

    def out_part(n):
        return _dot(seen[...], wo[n])

    def pass_on(b, t):
        return send(pp_out.at[t], pp_in.at[b * half + t], pp_s.at[t], pp_r.at[b * half + t], mate)

    def scatter(b, t):
        return send(rs_out.at[b * half + t], rs_in.at[core * half + t], rs_s.at[b * half + t], rs_r.at[core * half + t], far + b)

    def give(b):
        def mates(t, _):
            if b:
                pass_on(0, t).wait_send()
            pp_out[t] = out_part((1 - core) * half + t).astype(BF16)
            pass_on(b, t).start()
            return 0

        def mine(t, _):
            got = out_part(core * half + t)
            pass_on(b, t).wait_recv()
            rs_out[b * half + t] = (got + pp_in[b * half + t].astype(F32)).astype(BF16)
            scatter(b, t).start()
            return 0

        lax.fori_loop(0, half, mates, 0)
        lax.fori_loop(0, half, mine, 0)

    def last(n):
        return send(fin_out(n), fin_in.at[n], fin_s.at[n], fin_r.at[n], mate)

    def place(i):
        return (i % 2) * half + i // 2

    def mates_rows(i, _):
        n = place(i)
        fin_out(n)[...] = out_part(n).astype(BF16)
        last(n).start()
        return 0

    def my_rows(t, _):
        for h in range(2):
            n = h * half + t
            got = out_part(n)
            last(n).wait_recv()
            mine = xs[me, :, :, pl.ds(pl.multiple_of(n * TILE, TILE), TILE)].reshape(rows, TILE).astype(F32)
            mix[h * rows : (h + 1) * rows, :] = mine + (got + fin_in[n].astype(F32))
        for h in range(2):
            n = h * half + t
            send(rs_out.at[0], rs_in.at[n], rs_s.at[0], rs_r.at[n], peer).wait_recv()
            y[:, pl.ds(pl.multiple_of(n * TILE, TILE), TILE)] = (mix[h * rows : (h + 1) * rows, :] + rs_in[n].astype(F32)).astype(BF16)
        return 0

    for n in range(3):
        local_x(n).start()
    for copy in small:
        copy.start()
    for n in range(nq):
        weights_q(n).start()
    barrier = pltpu.get_barrier_semaphore()
    for to in (mate, peer, (mate + 2) % 4):
        pl.semaphore_signal(barrier, 1, device_id={"tp": to}, device_id_type=pl.DeviceIdType.MESH)
    pl.semaphore_wait(barrier, 3)
    own(0).start()
    own(1).start()
    local_x(0).wait()

    @pl.when(core == 0)
    def _():
        gather(0).start()

    local_x(1).wait()

    @pl.when(core == 0)
    def _():
        gather(1).start()
        gather(2).start()

    own(0).wait_recv()

    @pl.when(core == 1)
    def _():
        for m in range(3):
            gather(m).start()

    gather(3).start()
    gather(4).start()

    gap[...] = lax.rem(lax.broadcasted_iota(jnp.int32, gap.shape, 1), rows) - lax.broadcasted_iota(jnp.int32, gap.shape, 0)
    vt[:, :, HEAD:, :] = jnp.ones((4, kv, vt.shape[2] - HEAD, rows), BF16)

    local_x(2).wait()
    small[0].wait()
    gain_w[...] = gain[...].astype(F32)
    norm(me)
    small[1].wait()
    project(me, True)
    for n in range(no):
        weights_o(n).start()
    own(1).wait_recv()
    norm(mate)
    project(mate, False)

    for b in range(2):
        for m in ((0, 1, 2), (4,))[b]:
            gather(m).wait_recv()
            relay(m).start()
        for m in ((0, 1, 2), (3, 4))[b]:
            relay(m).wait_recv()
        norm(far + b)
        project(far + b, False)
        attend(far + b)
        if b == 0:
            gather(3).wait_recv()
            relay(3).start()
            for n in range(no):
                weights_o(n).wait()
        give(b)

    attend(mate)
    lax.fori_loop(0, no, mates_rows, 0)
    attend(me)
    lax.fori_loop(0, half, my_rows, 0)

    for n in range(2):
        own(n).wait_send()
    for m in range(5):
        gather(m).wait_send()
        relay(m).wait_send()
    for t in range(half):
        pass_on(1, t).wait_send()
    for n in range(no):
        scatter(n // half, n % half).wait_send()
        last(n).wait_send()


def _table(tokens):
    half = HEAD // 2
    angle = np.arange(tokens, dtype=np.float32)[:, None] * np.float32(THETA) ** (-np.arange(half, dtype=np.float32) / np.float32(half))
    angle = angle.astype(np.float64)
    return np.concatenate([np.cos(angle), np.sin(angle)], -1).astype(np.float32)


def solution(mesh):
    def step(x, gain, wq, wk, wv, wo):
        rows, d = x.shape
        heads, kv = wq.shape[1] // HEAD, wk.shape[1] // HEAD
        nq, no = wq.shape[1] // TILE, d // TILE
        strips = heads * rows // STRIP
        dma = lambda n: pltpu.SemaphoreType.DMA((n,))
        vm = pltpu.VMEM
        tokens = 4 * rows
        return pl.pallas_call(
            _layer,
            out_shape=pltpu.VMEM((rows, d), BF16),
            in_specs=[pl.BlockSpec(memory_space=pl.ANY)] * 7,
            out_specs=pl.BlockSpec(memory_space=pltpu.VMEM),
            scratch_shapes=[
                vm((nq, d, TILE), BF16), vm((d, 2 * kv * HEAD), BF16), vm((no, heads * HEAD, TILE), BF16),
                vm((4, rows // 16, 16, d), BF16), vm((rows, d), BF16), vm((d // 128, 128), BF16), vm((d // 128, 128), F32), vm((tokens, HEAD), F32), vm((2, rows, HEAD), F32),
                vm((4, heads, rows, HEAD), BF16), vm((4, kv, rows, HEAD), BF16), vm((4, kv, HEAD + 16, rows), BF16),
                vm((strips, STRIP), F32), vm((strips * (HEAD + 16), STRIP), F32), vm((rows, STRIP), jnp.int32), vm((rows, heads * HEAD), BF16),
                vm((no // 2, rows, TILE), BF16), vm((no, rows, TILE), BF16), vm((no, rows, TILE), BF16), vm((no, rows, TILE), BF16),
                vm((no, rows, TILE), BF16),
                dma(7 + nq), dma(no), dma(2), dma(2), dma(5), dma(5), dma(5), dma(5), dma(no // 2), dma(no), dma(no), dma(no),
                dma(no), dma(no),
            ],
            compiler_params=pltpu.CompilerParams(collective_id=0, has_side_effects=True, vmem_limit_bytes=247 * 2**18),
            cost_estimate=pl.CostEstimate(flops=33 * 10**9, bytes_accessed=34 * 2**20, transcendentals=8 * 2**20),
            name="layer",
        )(x.reshape(rows // 16, 16, d), gain.reshape(d // 128, 128), jnp.asarray(_table(tokens)), wq, wk, wv, wo)

    tokens, columns = P(("dp", "tp"), None), P(None, "tp")
    return jax.shard_map(
        step,
        mesh=mesh,
        in_specs=(tokens, P(None), columns, columns, columns, P("tp", None)),
        out_specs=tokens,
        check_vma=False,
    )
```

```python
import functools

import jax
import jax.numpy as jnp
import numpy as np
from jax import lax
from jax.experimental import pallas as pl
from jax.experimental.pallas import tpu as pltpu
from jax.sharding import PartitionSpec as P

HEAD = 128
THETA = 10000
NEG = -1e30
HIDDEN = 2 * NEG
LOG2E = 1.4426950408889634
TILE = 512
STRIP = 512
F32, BF16 = jnp.float32, jnp.bfloat16


def _dot(a, b, ca=1, cb=0):
    return lax.dot_general(a, b, (((ca,), (cb,)), ((), ())), preferred_element_type=F32)


def _layer(x_hbm, gain_hbm, tab_hbm, wq_hbm, wk_hbm, wv_hbm, wo_hbm, y,
           wq, wkv, wo, xs, a, gain, gain_w, tab, rope, q, k, vt, top, mix, gap, seen, pp_out, pp_in, rs_out, rs_in, fin_in,
           ld, own_s, own_r, ag_s, ag_r, rl_s, rl_r, pp_r, rs_r):
    me = lax.axis_index("tp")
    chip, core = me // 2, me % 2
    mate, peer = chip * 2 + 1 - core, (me + 2) % 4
    base, far = chip * 2, 2 - chip * 2
    rows = a.shape[0]
    d = a.shape[1]
    nq, no = wq.shape[0], wo.shape[0]
    heads, kv = q.shape[1], k.shape[1]
    group = heads // kv
    per = STRIP // rows
    half = no // 2
    hu = xs.shape[1] // 2

    def fin_out(n):
        return wq.at[1, pl.ds(pl.multiple_of(n * rows, rows), rows)]

    def send(src, dst, s, r, to):
        return pltpu.make_async_remote_copy(src, dst, s, r, device_id={"tp": to}, device_id_type=pl.DeviceIdType.MESH)

    wo_ld, pp_s, fin_s, rs_s, fin_r = ld.at[0], ld.at[1], ld.at[2], (ld.at[3], ld.at[4]), own_r.at[0]

    def all_of(ref, sem):
        return pltpu.make_async_copy(ref, ref, sem)

    def local_x(n):
        h = core if n < 2 else 1 - core
        at = pl.ds(h * hu + (n == 1), (1, hu - 1, hu)[n])
        return pltpu.make_async_copy(x_hbm.at[at], xs.at[me, at], ld.at[n])

    def own(n):
        at = pl.ds((1 - core if n == 0 else core) * hu, hu)
        return send(x_hbm.at[at], xs.at[me, at], own_s.at[0], own_r.at[n], mate)

    def message(m, first):
        blk, at, n = ((0, 0, 1), (0, 1, hu // 2 - 1), (0, hu // 2, hu // 2), (1, 0, hu // 2), (1, hu // 2, hu // 2))[m]
        return xs.at[first + blk, pl.ds(core * hu + at, n)]

    def gather(m):
        at = message(m, base)
        return send(at, at, ag_s.at[0], ag_r.at[m], peer)

    def relay(m):
        at = message(m, far)
        return send(at, at, rl_s.at[0], rl_r.at[m], mate)

    def weights_q(n):
        return pltpu.make_async_copy(wq_hbm.at[:, pl.ds(pl.multiple_of(n * TILE, TILE), TILE)], wq.at[n], ld.at[6 + n])

    def weights_o(n):
        return pltpu.make_async_copy(wo_hbm.at[:, pl.ds(pl.multiple_of(n * TILE, TILE), TILE)], wo.at[n], wo_ld)

    wide = kv * HEAD
    small = [
        pltpu.make_async_copy(gain_hbm, gain, ld.at[3]),
        pltpu.make_async_copy(tab_hbm, tab, ld.at[4]),
        pltpu.make_async_copy(wk_hbm, wkv.at[:, pl.ds(0, wide)], ld.at[5]),
        pltpu.make_async_copy(wv_hbm, wkv.at[:, pl.ds(wide, wide)], ld.at[5]),
    ]

    def norm(blk):
        step = 32
        units = step // xs.shape[2]

        def some(i, _):
            at = (blk, pl.ds(i * units, units))
            total = jnp.zeros((step, 128), F32)
            for c in range(0, d, 128):
                w = xs[(*at, slice(None), pl.ds(c, 128))].reshape(step, 128).astype(F32)
                total = total + w * w
            scale = lax.rsqrt(jnp.sum(total, axis=1, keepdims=True) * (1 / d) + 1e-6)
            for c in range(0, d, 128):
                w = xs[(*at, slice(None), pl.ds(c, 128))].reshape(step, 128).astype(F32)
                a[pl.ds(pl.multiple_of(i * step, step), step), pl.ds(c, 128)] = (w * scale * gain_w[pl.ds(c // 128, 1), :]).astype(BF16)
            return 0

        lax.fori_loop(0, rows // step, some, 0)

    def turned(t):
        t = t.astype(BF16).astype(F32)
        return (t * rope[0] + pltpu.roll(t, HEAD // 2, 1) * rope[1]).astype(BF16)

    def project(blk, loading):
        t = tab[pl.ds(pl.multiple_of(blk * rows, rows), rows), :]
        r = pltpu.roll(t, HEAD // 2, 1)
        first = lax.broadcasted_iota(jnp.int32, t.shape, 1) < HEAD // 2
        rope[0] = jnp.where(first, t, r)
        rope[1] = jnp.where(first, -r, t)
        if loading:
            all_of(wkv, ld.at[5]).wait()
        got = _dot(a[...], wkv[...])
        for i in range(kv):
            k[blk, i] = turned(got[:, i * HEAD : (i + 1) * HEAD])
            vt[blk, i, :HEAD, :] = got[:, wide + i * HEAD : wide + (i + 1) * HEAD].T.astype(BF16)

        def some(n, _):
            if loading:
                weights_q(n).wait()
            got = _dot(a[...], wq[n])
            for i in range(TILE // HEAD):
                q[blk, n * (TILE // HEAD) + i] = turned(got[:, i * HEAD : (i + 1) * HEAD])
            return 0

        lax.fori_loop(0, nq, some, 0)

    def attend(blk):
        e = HEAD**-0.5 * LOG2E
        deep = vt.shape[2]
        pieces = [(i, i * group + n) for i in range(kv) for n in range(0, group, per)]
        top[...] = jnp.full(top.shape, NEG, F32)
        mix[...] = jnp.zeros(mix.shape, F32)

        def block(j, masked):
            scores = [_dot(k[j, i], q[blk, pl.ds(n, per)].reshape(STRIP, HEAD), 1, 1) for i, n in pieces]
            weights, keeps = [], []
            for p, s in enumerate(scores):
                if masked:
                    s = jnp.where(gap[...] >= 0, s, HIDDEN)
                old = top[p : p + 1, :]
                new = jnp.maximum(old, s.max(axis=0, keepdims=True))
                top[p : p + 1, :] = new
                weights.append(jnp.exp2((s - new) * e).astype(BF16))
                keeps.append(jnp.exp2((old - new) * e))
            for p, (w, keep) in enumerate(zip(weights, keeps)):
                at = pl.ds(p * deep, deep)
                mix[at, :] = mix[at, :] * keep + _dot(vt[j, pieces[p][0]], w)

        lax.fori_loop(0, blk, lambda j, _: (block(j, False), 0)[1], 0)
        block(blk, True)
        for p, (i, n) in enumerate(pieces):
            got = mix[p * deep : p * deep + HEAD, :] * (1 / mix[p * deep + HEAD : p * deep + HEAD + 1, :])
            for m in range(per):
                seen[:, (n + m) * HEAD : (n + m + 1) * HEAD] = got[:, m * rows : (m + 1) * rows].T.astype(BF16)

    def out_part(n):
        return _dot(seen[...], wo[n])

    def pass_on(b, t):
        return send(pp_out.at[t], pp_in.at[b * half + t], pp_s, pp_r.at[t], mate)

    def scatter(b, t):
        return send(rs_out.at[b * half + t], rs_in.at[t, core], rs_s[b], rs_r.at[t], far + b)

    def give(b):
        def mates(t, _):
            pp_out[t] = out_part((1 - core) * half + t).astype(BF16)
            pass_on(b, t).start()
            return 0

        def mine(t, _):
            got = out_part(core * half + t)
            pass_on(b, t).wait_recv()
            rs_out[b * half + t] = (got + pp_in[b * half + t].astype(F32)).astype(BF16)
            scatter(b, t).start()
            return 0

        if b:
            all_of(pp_out, pp_s).wait()
        lax.fori_loop(0, half, mates, 0)
        lax.fori_loop(0, half, mine, 0)

    def last(n):
        return send(fin_out(n), fin_in.at[n], fin_s, fin_r, mate)

    def place(i):
        return (i % 2) * half + i // 2

    def mates_rows(i, _):
        n = place(i)
        fin_out(n)[...] = out_part(n).astype(BF16)
        last(n).start()
        return 0

    def my_rows(t, _):
        for h in range(2):
            n = h * half + t
            got = out_part(n)
            mine = xs[me, :, :, pl.ds(pl.multiple_of(n * TILE, TILE), TILE)].reshape(rows, TILE).astype(F32)
            mix[h * rows : (h + 1) * rows, :] = mine + (got + fin_in[n].astype(F32))
        all_of(rs_in.at[t], rs_r.at[t]).wait()
        for h in range(2):
            at = pl.ds(pl.multiple_of((h * half + t) * TILE, TILE), TILE)
            y[:, at] = (mix[h * rows : (h + 1) * rows, :] + rs_in[t, h].astype(F32)).astype(BF16)
        return 0

    for n in range(3):
        local_x(n).start()
    for copy in small:
        copy.start()
    for n in range(nq):
        weights_q(n).start()
    barrier = pltpu.get_barrier_semaphore()
    for to in (mate, peer, (mate + 2) % 4):
        pl.semaphore_signal(barrier, 1, device_id={"tp": to}, device_id_type=pl.DeviceIdType.MESH)
    pl.semaphore_wait(barrier, 3)
    own(0).start()
    own(1).start()
    local_x(0).wait()

    @pl.when(core == 0)
    def _():
        gather(0).start()

    local_x(1).wait()

    @pl.when(core == 0)
    def _():
        gather(1).start()
        gather(2).start()

    own(0).wait_recv()

    @pl.when(core == 1)
    def _():
        for m in range(3):
            gather(m).start()

    gather(3).start()
    gather(4).start()

    gap[...] = lax.rem(lax.broadcasted_iota(jnp.int32, gap.shape, 1), rows) - lax.broadcasted_iota(jnp.int32, gap.shape, 0)
    vt[:, :, HEAD:, :] = jnp.ones((4, kv, vt.shape[2] - HEAD, rows), BF16)

    local_x(2).wait()
    small[0].wait()
    gain_w[...] = gain[...].astype(F32)
    norm(me)
    small[1].wait()
    project(me, True)
    for n in range(no):
        weights_o(n).start()
    own(1).wait_recv()
    norm(mate)
    project(mate, False)

    for b in range(2):
        for m in ((0, 1, 2), (4,))[b]:
            gather(m).wait_recv()
            relay(m).start()
        for m in ((0, 1, 2), (3, 4))[b]:
            relay(m).wait_recv()
        norm(far + b)
        project(far + b, False)
        attend(far + b)
        if b == 0:
            gather(3).wait_recv()
            relay(3).start()
            all_of(wo, wo_ld).wait()
        give(b)

    attend(mate)
    lax.fori_loop(0, no, mates_rows, 0)
    attend(me)

    for sem in (own_s, ag_s, rl_s):
        all_of(xs.at[0], sem.at[0]).wait()
    all_of(pp_out, pp_s).wait()
    all_of(fin_in, fin_s).wait()
    all_of(pp_out, rs_s[0]).wait()
    all_of(fin_in, fin_r).wait()

    lax.fori_loop(0, half, my_rows, 0)

    all_of(pp_out, rs_s[1]).wait()


def _table(tokens):
    half = HEAD // 2
    angle = np.arange(tokens, dtype=np.float32)[:, None] * np.float32(THETA) ** (-np.arange(half, dtype=np.float32) / np.float32(half))
    angle = angle.astype(np.float64)
    return np.concatenate([np.cos(angle), np.sin(angle)], -1).astype(np.float32)


def solution(mesh):
    def step(x, gain, wq, wk, wv, wo):
        rows, d = x.shape
        heads, kv = wq.shape[1] // HEAD, wk.shape[1] // HEAD
        nq, no = wq.shape[1] // TILE, d // TILE
        strips = heads * rows // STRIP
        dma = lambda n: pltpu.SemaphoreType.DMA((n,))
        vm = pltpu.VMEM
        tokens = 4 * rows
        return pl.pallas_call(
            _layer,
            out_shape=pltpu.VMEM((rows, d), BF16),
            in_specs=[pl.BlockSpec(memory_space=pl.ANY)] * 7,
            out_specs=pl.BlockSpec(memory_space=pltpu.VMEM),
            scratch_shapes=[
                vm((nq, d, TILE), BF16), vm((d, 2 * kv * HEAD), BF16), vm((no, heads * HEAD, TILE), BF16),
                vm((4, rows // 16, 16, d), BF16), vm((rows, d), BF16), vm((d // 128, 128), BF16), vm((d // 128, 128), F32), vm((tokens, HEAD), F32), vm((2, rows, HEAD), F32),
                vm((4, heads, rows, HEAD), BF16), vm((4, kv, rows, HEAD), BF16), vm((4, kv, HEAD + 16, rows), BF16),
                vm((strips, STRIP), F32), vm((strips * (HEAD + 16), STRIP), F32), vm((rows, STRIP), jnp.int32), vm((rows, heads * HEAD), BF16),
                vm((no // 2, rows, TILE), BF16), vm((no, rows, TILE), BF16), vm((no, rows, TILE), BF16), vm((no // 2, 2, rows, TILE), BF16),
                vm((no, rows, TILE), BF16),
                dma(6 + nq), dma(1), dma(2), dma(1), dma(5), dma(1), dma(5), dma(no // 2), dma(no // 2),
            ],
            compiler_params=pltpu.CompilerParams(collective_id=0, has_side_effects=True, vmem_limit_bytes=247 * 2**18),
            cost_estimate=pl.CostEstimate(flops=33 * 10**9, bytes_accessed=34 * 2**20, transcendentals=8 * 2**20),
            name="layer",
        )(x.reshape(rows // 16, 16, d), gain.reshape(d // 128, 128), jnp.asarray(_table(tokens)), wq, wk, wv, wo)

    tokens, columns = P(("dp", "tp"), None), P(None, "tp")
    return jax.shard_map(
        step,
        mesh=mesh,
        in_specs=(tokens, P(None), columns, columns, columns, P("tp", None)),
        out_specs=tokens,
        check_vma=False,
    )
```

```python
import functools

import jax
import jax.numpy as jnp
import numpy as np
from jax import lax
from jax.experimental import pallas as pl
from jax.experimental.pallas import tpu as pltpu
from jax.sharding import PartitionSpec as P

HEAD = 128
THETA = 10000
NEG = -1e30
HIDDEN = 2 * NEG
LOG2E = 1.4426950408889634
TILE = 512
STRIP = 512
F32, BF16 = jnp.float32, jnp.bfloat16


def _dot(a, b, ca=1, cb=0):
    return lax.dot_general(a, b, (((ca,), (cb,)), ((), ())), preferred_element_type=F32)


def _layer(x_hbm, gain_hbm, tab_hbm, wq_hbm, wk_hbm, wv_hbm, wo_hbm, y,
           wq, wkv, wo, xs, a, gain, gain_w, tab, rope, q, k, vt, top, mix, gap, seen, pp_out, pp_in, rs_out, rs_in, fin_in,
           ld, own_s, own_r, ag_s, ag_r, rl_s, rl_r, pp_r, rs_r):
    me = lax.axis_index("tp")
    chip, core = me // 2, me % 2
    mate, peer = chip * 2 + 1 - core, (me + 2) % 4
    base, far = chip * 2, 2 - chip * 2
    rows = a.shape[0]
    d = a.shape[1]
    nq, no = wq.shape[0], wo.shape[0]
    heads, kv = q.shape[1], k.shape[1]
    group = heads // kv
    per = STRIP // rows
    half = no // 2
    hu = xs.shape[1] // 2

    def fin_out(n):
        return wq.at[1, pl.ds(pl.multiple_of(n * rows, rows), rows)]

    def send(src, dst, s, r, to):
        return pltpu.make_async_remote_copy(src, dst, s, r, device_id={"tp": to}, device_id_type=pl.DeviceIdType.MESH)

    wo_ld, pp_s, fin_s, rs_s, fin_r = ld.at[0], ld.at[1], ld.at[2], (ld.at[3], ld.at[4]), own_r.at[0]

    def all_of(ref, sem):
        return pltpu.make_async_copy(ref, ref, sem)

    def local_x(n):
        h = core if n < 2 else 1 - core
        at = pl.ds(h * hu + (n == 1), (1, hu - 1, hu)[n])
        return pltpu.make_async_copy(x_hbm.at[at], xs.at[me, at], ld.at[n])

    def own(n):
        at = pl.ds((1 - core if n == 0 else core) * hu, hu)
        return send(x_hbm.at[at], xs.at[me, at], own_s.at[0], own_r.at[n], mate)

    def gather(p):
        blk, at, n, m = ((0, 0, 1, 0), (0, 1, hu // 2 - 1, 0), (0, hu // 2, hu // 2, 1), (1, 0, 1, 2), (1, 1, hu // 2 - 1, 2), (1, hu // 2, hu // 2, 3))[p]
        at = xs.at[base + blk, pl.ds(core * hu + at, n)]
        return send(at, at, ag_s.at[0], ag_r.at[m], peer)

    def quarter(m):
        return xs.at[far + m // 2, pl.ds(core * hu + m % 2 * (hu // 2), hu // 2)]

    def relay(m):
        return send(quarter(m), quarter(m), rl_s.at[0], rl_r.at[m], mate)

    def relays(ms):
        for m in ms:
            all_of(quarter(m), ag_r.at[m]).wait()
            relay(m).start()

    def weights_q(n):
        return pltpu.make_async_copy(wq_hbm.at[:, pl.ds(pl.multiple_of(n * TILE, TILE), TILE)], wq.at[n], ld.at[6 + n])

    def weights_o(n):
        return pltpu.make_async_copy(wo_hbm.at[:, pl.ds(pl.multiple_of(n * TILE, TILE), TILE)], wo.at[n], wo_ld)

    wide = kv * HEAD
    small = [
        pltpu.make_async_copy(gain_hbm, gain, ld.at[3]),
        pltpu.make_async_copy(tab_hbm, tab, ld.at[4]),
        pltpu.make_async_copy(wk_hbm, wkv.at[:, pl.ds(0, wide)], ld.at[5]),
        pltpu.make_async_copy(wv_hbm, wkv.at[:, pl.ds(wide, wide)], ld.at[5]),
    ]

    def norm(blk):
        step = 32
        units = step // xs.shape[2]

        def some(i, _):
            at = (blk, pl.ds(i * units, units))
            total = jnp.zeros((step, 128), F32)
            for c in range(0, d, 128):
                w = xs[(*at, slice(None), pl.ds(c, 128))].reshape(step, 128).astype(F32)
                total = total + w * w
            scale = lax.rsqrt(jnp.sum(total, axis=1, keepdims=True) * (1 / d) + 1e-6)
            for c in range(0, d, 128):
                w = xs[(*at, slice(None), pl.ds(c, 128))].reshape(step, 128).astype(F32)
                a[pl.ds(pl.multiple_of(i * step, step), step), pl.ds(c, 128)] = (w * scale * gain_w[pl.ds(c // 128, 1), :]).astype(BF16)
            return 0

        lax.fori_loop(0, rows // step, some, 0)

    def turned(t):
        t = t.astype(BF16).astype(F32)
        return (t * rope[0] + pltpu.roll(t, HEAD // 2, 1) * rope[1]).astype(BF16)

    def project(blk, loading):
        t = tab[pl.ds(pl.multiple_of(blk * rows, rows), rows), :]
        r = pltpu.roll(t, HEAD // 2, 1)
        first = lax.broadcasted_iota(jnp.int32, t.shape, 1) < HEAD // 2
        rope[0] = jnp.where(first, t, r)
        rope[1] = jnp.where(first, -r, t)
        if loading:
            all_of(wkv, ld.at[5]).wait()
        got = _dot(a[...], wkv[...])
        for i in range(kv):
            k[blk, i] = turned(got[:, i * HEAD : (i + 1) * HEAD])
            vt[blk, i, :HEAD, :] = got[:, wide + i * HEAD : wide + (i + 1) * HEAD].T.astype(BF16)

        def some(n, _):
            if loading:
                weights_q(n).wait()
            got = _dot(a[...], wq[n])
            for i in range(TILE // HEAD):
                q[blk, n * (TILE // HEAD) + i] = turned(got[:, i * HEAD : (i + 1) * HEAD])
            return 0

        lax.fori_loop(0, nq, some, 0)

    def attend(blk):
        e = HEAD**-0.5 * LOG2E
        deep = vt.shape[2]
        pieces = [(i, i * group + n) for i in range(kv) for n in range(0, group, per)]
        top[...] = jnp.full(top.shape, NEG, F32)
        mix[...] = jnp.zeros(mix.shape, F32)

        def block(j, masked):
            scores = [_dot(k[j, i], q[blk, pl.ds(n, per)].reshape(STRIP, HEAD), 1, 1) for i, n in pieces]
            weights, keeps = [], []
            for p, s in enumerate(scores):
                if masked:
                    s = jnp.where(gap[...] >= 0, s, HIDDEN)
                old = top[p : p + 1, :]
                new = jnp.maximum(old, s.max(axis=0, keepdims=True))
                top[p : p + 1, :] = new
                weights.append(jnp.exp2((s - new) * e).astype(BF16))
                keeps.append(jnp.exp2((old - new) * e))
            for p, (w, keep) in enumerate(zip(weights, keeps)):
                at = pl.ds(p * deep, deep)
                mix[at, :] = mix[at, :] * keep + _dot(vt[j, pieces[p][0]], w)

        lax.fori_loop(0, blk, lambda j, _: (block(j, False), 0)[1], 0)
        block(blk, True)
        for p, (i, n) in enumerate(pieces):
            got = mix[p * deep : p * deep + HEAD, :] * (1 / mix[p * deep + HEAD : p * deep + HEAD + 1, :])
            for m in range(per):
                seen[:, (n + m) * HEAD : (n + m + 1) * HEAD] = got[:, m * rows : (m + 1) * rows].T.astype(BF16)

    def out_part(n):
        return _dot(seen[...], wo[n])

    def pass_on(b, t):
        return send(pp_out.at[t], pp_in.at[b * half + t], pp_s, pp_r.at[t], mate)

    def scatter(b, t):
        return send(rs_out.at[b * half + t], rs_in.at[t, core], rs_s[b], rs_r.at[t], far + b)

    def give(b):
        def mates(t):
            pp_out[t] = out_part((1 - core) * half + t).astype(BF16)
            pass_on(b, t).start()

        def mine(t):
            got = out_part(core * half + t)
            pass_on(b, t).wait_recv()
            rs_out[b * half + t] = (got + pp_in[b * half + t].astype(F32)).astype(BF16)
            scatter(b, t).start()

        def both(t, _):
            mates(t + 1)
            mine(t)
            return 0

        if b:
            all_of(pp_out, pp_s).wait()
        mates(0)
        lax.fori_loop(0, half - 1, both, 0)
        mine(half - 1)

    def last(n):
        return send(fin_out(n), fin_in.at[n], fin_s, fin_r, mate)

    def place(i):
        return (i % 2) * half + i // 2

    def mates_rows(i, _):
        n = place(i)
        fin_out(n)[...] = out_part(n).astype(BF16)
        last(n).start()
        return 0

    def my_rows(t, _):
        for h in range(2):
            n = h * half + t
            got = out_part(n)
            mine = xs[me, :, :, pl.ds(pl.multiple_of(n * TILE, TILE), TILE)].reshape(rows, TILE).astype(F32)
            mix[h * rows : (h + 1) * rows, :] = mine + (got + fin_in[n].astype(F32))
        all_of(rs_in.at[t], rs_r.at[t]).wait()
        for h in range(2):
            at = pl.ds(pl.multiple_of((h * half + t) * TILE, TILE), TILE)
            y[:, at] = (mix[h * rows : (h + 1) * rows, :] + rs_in[t, h].astype(F32)).astype(BF16)
        return 0

    for n in range(3):
        local_x(n).start()
    for copy in small:
        copy.start()
    for n in range(nq):
        weights_q(n).start()
    barrier = pltpu.get_barrier_semaphore()
    for to in (mate, peer, (mate + 2) % 4):
        pl.semaphore_signal(barrier, 1, device_id={"tp": to}, device_id_type=pl.DeviceIdType.MESH)
    pl.semaphore_wait(barrier, 3)
    own(0).start()
    own(1).start()
    local_x(0).wait()

    @pl.when(core == 0)
    def _():
        gather(0).start()

    @pl.when(core == 1)
    def _():
        gather(3).start()

    local_x(1).wait()

    @pl.when(core == 0)
    def _():
        gather(1).start()
        gather(2).start()

    own(0).wait_recv()

    @pl.when(core == 0)
    def _():
        gather(3).start()

    @pl.when(core == 1)
    def _():
        for p in range(3):
            gather(p).start()

    gather(4).start()
    gather(5).start()

    gap[...] = lax.rem(lax.broadcasted_iota(jnp.int32, gap.shape, 1), rows) - lax.broadcasted_iota(jnp.int32, gap.shape, 0)
    vt[:, :, HEAD:, :] = jnp.ones((4, kv, vt.shape[2] - HEAD, rows), BF16)

    local_x(2).wait()
    small[0].wait()
    gain_w[...] = gain[...].astype(F32)
    norm(me)
    small[1].wait()
    project(me, True)
    for n in range(no):
        weights_o(n).start()
    own(1).wait_recv()
    norm(mate)
    project(mate, False)

    for b in range(2):
        relays(((0, 1), (3,))[b])
        for m in (2 * b, 2 * b + 1):
            relay(m).wait_recv()
        norm(far + b)
        project(far + b, False)
        attend(far + b)
        if b == 0:
            relays((2,))
            all_of(wo, wo_ld).wait()
        give(b)

    attend(mate)
    lax.fori_loop(0, no, mates_rows, 0)
    attend(me)

    for sem in (own_s, ag_s, rl_s):
        all_of(xs.at[0], sem.at[0]).wait()
    all_of(pp_out, pp_s).wait()
    all_of(fin_in, fin_s).wait()
    all_of(pp_out, rs_s[0]).wait()
    all_of(fin_in, fin_r).wait()

    lax.fori_loop(0, half, my_rows, 0)

    all_of(pp_out, rs_s[1]).wait()


def _table(tokens):
    half = HEAD // 2
    angle = np.arange(tokens, dtype=np.float32)[:, None] * np.float32(THETA) ** (-np.arange(half, dtype=np.float32) / np.float32(half))
    angle = angle.astype(np.float64)
    return np.concatenate([np.cos(angle), np.sin(angle)], -1).astype(np.float32)


def solution(mesh):
    def step(x, gain, wq, wk, wv, wo):
        rows, d = x.shape
        heads, kv = wq.shape[1] // HEAD, wk.shape[1] // HEAD
        nq, no = wq.shape[1] // TILE, d // TILE
        strips = heads * rows // STRIP
        dma = lambda n: pltpu.SemaphoreType.DMA((n,))
        vm = pltpu.VMEM
        tokens = 4 * rows
        return pl.pallas_call(
            _layer,
            out_shape=pltpu.VMEM((rows, d), BF16),
            in_specs=[pl.BlockSpec(memory_space=pl.ANY)] * 7,
            out_specs=pl.BlockSpec(memory_space=pltpu.VMEM),
            scratch_shapes=[
                vm((nq, d, TILE), BF16), vm((d, 2 * kv * HEAD), BF16), vm((no, heads * HEAD, TILE), BF16),
                vm((4, rows // 16, 16, d), BF16), vm((rows, d), BF16), vm((d // 128, 128), BF16), vm((d // 128, 128), F32), vm((tokens, HEAD), F32), vm((2, rows, HEAD), F32),
                vm((4, heads, rows, HEAD), BF16), vm((4, kv, rows, HEAD), BF16), vm((4, kv, HEAD + 16, rows), BF16),
                vm((strips, STRIP), F32), vm((strips * (HEAD + 16), STRIP), F32), vm((rows, STRIP), jnp.int32), vm((rows, heads * HEAD), BF16),
                vm((no // 2, rows, TILE), BF16), vm((no, rows, TILE), BF16), vm((no, rows, TILE), BF16), vm((no // 2, 2, rows, TILE), BF16),
                vm((no, rows, TILE), BF16),
                dma(6 + nq), dma(1), dma(2), dma(1), dma(4), dma(1), dma(4), dma(no // 2), dma(no // 2),
            ],
            compiler_params=pltpu.CompilerParams(collective_id=0, has_side_effects=True, vmem_limit_bytes=247 * 2**18),
            cost_estimate=pl.CostEstimate(flops=33 * 10**9, bytes_accessed=34 * 2**20, transcendentals=8 * 2**20),
            name="layer",
        )(x.reshape(rows // 16, 16, d), gain.reshape(d // 128, 128), jnp.asarray(_table(tokens)), wq, wk, wv, wo)

    tokens, columns = P(("dp", "tp"), None), P(None, "tp")
    return jax.shard_map(
        step,
        mesh=mesh,
        in_specs=(tokens, P(None), columns, columns, columns, P("tp", None)),
        out_specs=tokens,
        check_vma=False,
    )
```

```python
import functools

import jax
import jax.numpy as jnp
import numpy as np
from jax import lax
from jax.experimental import pallas as pl
from jax.experimental.pallas import tpu as pltpu
from jax.sharding import PartitionSpec as P

HEAD = 128
THETA = 10000
LOWEST = float(np.finfo(np.float32).min)
LOG2E = 1.4426950408889634
TILE = 512
STRIP = 512
F32, BF16 = jnp.float32, jnp.bfloat16


def _dot(a, b, ca=1, cb=0):
    return lax.dot_general(a, b, (((ca,), (cb,)), ((), ())), preferred_element_type=F32)


def _layer(x_hbm, gain_hbm, tab_hbm, wq_hbm, wk_hbm, wv_hbm, wo_hbm, y,
           wq, wkv, wo, xs, a, gain, gain_w, tab, rope, q, k, vt, top, mix, gap, seen, pp_out, pp_in, rs_out, rs_in, fin_in,
           ld, own_r, xs_s, ag_r, rl_r, pp_r, rs_r):
    me = lax.axis_index("tp")
    chip, core = me // 2, me % 2
    mate, peer = chip * 2 + 1 - core, (me + 2) % 4
    base, far = chip * 2, 2 - chip * 2
    rows = a.shape[0]
    d = a.shape[1]
    nq, no = wq.shape[0], wo.shape[0]
    heads, kv = q.shape[1], k.shape[1]
    group = heads // kv
    per = STRIP // rows
    half = no // 2
    hu = xs.shape[1] // 2

    def fin_out(n):
        return wq.at[1, pl.ds(pl.multiple_of(n * rows, rows), rows)]

    def send(src, dst, s, r, to):
        return pltpu.make_async_remote_copy(src, dst, s, r, device_id={"tp": to}, device_id_type=pl.DeviceIdType.MESH)

    wo_ld, pp_s, fin_s, rs_s, fin_r = ld.at[0], ld.at[1], ld.at[2], (ld.at[3], ld.at[4]), own_r.at[0]

    def all_of(ref, sem):
        return pltpu.make_async_copy(ref, ref, sem)

    def local_x(n):
        h = core if n < 2 else 1 - core
        at = pl.ds(h * hu + (n == 1), (1, hu - 1, hu)[n])
        return pltpu.make_async_copy(x_hbm.at[at], xs.at[me, at], ld.at[n])

    def own(n):
        at = pl.ds((1 - core if n == 0 else core) * hu, hu)
        return send(x_hbm.at[at], xs.at[me, at], xs_s.at[0], own_r.at[n], mate)

    def gather(p):
        blk, at, n, m = ((0, 0, 1, 0), (0, 1, hu // 2 - 1, 0), (0, hu // 2, hu // 2, 1), (1, 0, 1, 2), (1, 1, hu // 2 - 1, 2), (1, hu // 2, hu // 2, 3))[p]
        at = xs.at[base + blk, pl.ds(core * hu + at, n)]
        return send(at, at, xs_s.at[0], ag_r.at[m], peer)

    def quarter(m):
        return xs.at[far + m // 2, pl.ds(core * hu + m % 2 * (hu // 2), hu // 2)]

    def relay(m):
        return send(quarter(m), quarter(m), xs_s.at[0], rl_r.at[m // 2], mate)

    def relays(ms):
        for m in ms:
            all_of(quarter(m), ag_r.at[m]).wait()
            relay(m).start()

    def weights_q(n):
        return pltpu.make_async_copy(wq_hbm.at[:, pl.ds(pl.multiple_of(n * TILE, TILE), TILE)], wq.at[n], ld.at[6])

    def weights_o(n):
        return pltpu.make_async_copy(wo_hbm.at[:, pl.ds(pl.multiple_of(n * TILE, TILE), TILE)], wo.at[n], wo_ld)

    wide = kv * HEAD
    small = [
        pltpu.make_async_copy(gain_hbm, gain, ld.at[3]),
        pltpu.make_async_copy(tab_hbm, tab, ld.at[4]),
        pltpu.make_async_copy(wk_hbm, wkv.at[:, pl.ds(0, wide)], ld.at[5]),
        pltpu.make_async_copy(wv_hbm, wkv.at[:, pl.ds(wide, wide)], ld.at[5]),
    ]

    def norm(blk):
        step = 32
        units = step // xs.shape[2]

        def some(i, _):
            at = (blk, pl.ds(i * units, units))
            total = jnp.zeros((step, 128), F32)
            for c in range(0, d, 128):
                w = xs[(*at, slice(None), pl.ds(c, 128))].reshape(step, 128).astype(F32)
                total = total + w * w
            scale = lax.rsqrt(jnp.sum(total, axis=1, keepdims=True) * (1 / d) + 1e-6)
            for c in range(0, d, 128):
                w = xs[(*at, slice(None), pl.ds(c, 128))].reshape(step, 128).astype(F32)
                a[pl.ds(pl.multiple_of(i * step, step), step), pl.ds(c, 128)] = (w * scale * gain_w[pl.ds(c // 128, 1), :]).astype(BF16)
            return 0

        lax.fori_loop(0, rows // step, some, 0)

    def turned(t):
        t = t.astype(BF16).astype(F32)
        return (t * rope[0] + pltpu.roll(t, HEAD // 2, 1) * rope[1]).astype(BF16)

    def project(blk, loading):
        t = tab[pl.ds(pl.multiple_of(blk * rows, rows), rows), :]
        r = pltpu.roll(t, HEAD // 2, 1)
        first = lax.broadcasted_iota(jnp.int32, t.shape, 1) < HEAD // 2
        rope[0] = jnp.where(first, t, r)
        rope[1] = jnp.where(first, -r, t)
        if loading:
            all_of(wkv, ld.at[5]).wait()
        got = _dot(a[...], wkv[...])
        for i in range(kv):
            k[blk, i] = turned(got[:, i * HEAD : (i + 1) * HEAD])
            vt[blk, i, :HEAD, :] = got[:, wide + i * HEAD : wide + (i + 1) * HEAD].T.astype(BF16)

        if loading:
            all_of(wq, ld.at[6]).wait()

        def some(n, _):
            got = _dot(a[...], wq[n])
            for i in range(TILE // HEAD):
                q[blk, n * (TILE // HEAD) + i] = turned(got[:, i * HEAD : (i + 1) * HEAD])
            return 0

        lax.fori_loop(0, nq, some, 0)

    def attend(blk):
        e = HEAD**-0.5 * LOG2E
        deep = vt.shape[2]
        pieces = [(i, i * group + n) for i in range(kv) for n in range(0, group, per)]
        top[...] = jnp.full(top.shape, LOWEST, F32)
        mix[...] = jnp.zeros(mix.shape, F32)

        def block(j, masked):
            scores = [_dot(k[j, i], q[blk, pl.ds(n, per)].reshape(STRIP, HEAD), 1, 1) for i, n in pieces]
            weights, keeps = [], []
            for p, s in enumerate(scores):
                if masked:
                    s = jnp.where(gap[...] >= 0, s, LOWEST)
                old = top[p : p + 1, :]
                new = jnp.maximum(old, s.max(axis=0, keepdims=True))
                top[p : p + 1, :] = new
                weights.append(jnp.exp2((s - new) * e).astype(BF16))
                keeps.append(jnp.exp2((old - new) * e))
            for p, (w, keep) in enumerate(zip(weights, keeps)):
                at = pl.ds(p * deep, deep)
                mix[at, :] = mix[at, :] * keep + _dot(vt[j, pieces[p][0]], w)

        lax.fori_loop(0, blk, lambda j, _: (block(j, False), 0)[1], 0)
        block(blk, True)
        for p, (i, n) in enumerate(pieces):
            got = mix[p * deep : p * deep + HEAD, :] * (1 / mix[p * deep + HEAD : p * deep + HEAD + 1, :])
            for m in range(per):
                seen[:, (n + m) * HEAD : (n + m + 1) * HEAD] = got[:, m * rows : (m + 1) * rows].T.astype(BF16)

    def out_part(n):
        return _dot(seen[...], wo[n])

    def pass_on(b, t):
        return send(pp_out.at[t], pp_in.at[b * half + t], pp_s, pp_r.at[t], mate)

    def scatter(b, t):
        return send(rs_out.at[b * half + t], rs_in.at[t, core], rs_s[b], rs_r.at[t], far + b)

    def give(b):
        def mates(t):
            pp_out[t] = out_part((1 - core) * half + t).astype(BF16)
            pass_on(b, t).start()

        def mine(t):
            got = out_part(core * half + t)
            pass_on(b, t).wait_recv()
            rs_out[b * half + t] = (got + pp_in[b * half + t].astype(F32)).astype(BF16)
            scatter(b, t).start()

        def both(t, _):
            mates(t + 1)
            mine(t)
            return 0

        if b:
            all_of(pp_out, pp_s).wait()
        mates(0)
        lax.fori_loop(0, half - 1, both, 0)
        mine(half - 1)

    def last(n):
        return send(fin_out(n), fin_in.at[n], fin_s, fin_r, mate)

    def place(i):
        return (i % 2) * half + i // 2

    def mates_rows(i, _):
        n = place(i)
        fin_out(n)[...] = out_part(n).astype(BF16)
        last(n).start()
        return 0

    def my_rows(t, _):
        for h in range(2):
            n = h * half + t
            got = out_part(n)
            mine = xs[me, :, :, pl.ds(pl.multiple_of(n * TILE, TILE), TILE)].reshape(rows, TILE).astype(F32)
            mix[h * rows : (h + 1) * rows, :] = mine + (got + fin_in[n].astype(F32))
        all_of(rs_in.at[t], rs_r.at[t]).wait()
        for h in range(2):
            at = pl.ds(pl.multiple_of((h * half + t) * TILE, TILE), TILE)
            y[:, at] = (mix[h * rows : (h + 1) * rows, :] + rs_in[t, h].astype(F32)).astype(BF16)
        return 0

    for n in range(3):
        local_x(n).start()
    barrier = pltpu.get_barrier_semaphore()
    for to in (mate, peer, (mate + 2) % 4):
        pl.semaphore_signal(barrier, 1, device_id={"tp": to}, device_id_type=pl.DeviceIdType.MESH)
    pl.semaphore_wait(barrier, 3)
    own(0).start()
    own(1).start()
    local_x(0).wait()

    @pl.when(core == 0)
    def _():
        gather(0).start()

    @pl.when(core == 1)
    def _():
        gather(3).start()

    for copy in small:
        copy.start()
    for n in range(nq):
        weights_q(n).start()
    local_x(1).wait()

    @pl.when(core == 0)
    def _():
        gather(1).start()
        gather(2).start()

    own(0).wait_recv()

    @pl.when(core == 0)
    def _():
        gather(3).start()

    @pl.when(core == 1)
    def _():
        for p in range(3):
            gather(p).start()

    gather(4).start()
    gather(5).start()

    gap[...] = lax.rem(lax.broadcasted_iota(jnp.int32, gap.shape, 1), rows) - lax.broadcasted_iota(jnp.int32, gap.shape, 0)
    vt[:, :, HEAD:, :] = jnp.ones((4, kv, vt.shape[2] - HEAD, rows), BF16)

    local_x(2).wait()
    small[0].wait()
    gain_w[...] = gain[...].astype(F32)
    norm(me)
    small[1].wait()
    project(me, True)
    for n in range(no):
        weights_o(n).start()
    own(1).wait_recv()
    norm(mate)
    project(mate, False)

    for b in range(2):
        relays(((0, 1), (3,))[b])
        all_of(xs.at[far + b, pl.ds((1 - core) * hu, hu)], rl_r.at[b]).wait()
        norm(far + b)
        project(far + b, False)
        attend(far + b)
        if b == 0:
            relays((2,))
            all_of(wo, wo_ld).wait()
        give(b)

    attend(mate)
    lax.fori_loop(0, no, mates_rows, 0)
    attend(me)

    all_of(xs.at[pl.ds(0, 3)], xs_s.at[0]).wait()
    all_of(pp_out, pp_s).wait()
    all_of(fin_in, fin_s).wait()
    all_of(pp_out, rs_s[0]).wait()
    all_of(fin_in, fin_r).wait()

    lax.fori_loop(0, half, my_rows, 0)

    all_of(pp_out, rs_s[1]).wait()


def _table(tokens):
    half = HEAD // 2
    angle = np.arange(tokens, dtype=np.float32)[:, None] * np.float32(THETA) ** (-np.arange(half, dtype=np.float32) / np.float32(half))
    angle = angle.astype(np.float64)
    return np.concatenate([np.cos(angle), np.sin(angle)], -1).astype(np.float32)


def solution(mesh):
    def step(x, gain, wq, wk, wv, wo):
        rows, d = x.shape
        heads, kv = wq.shape[1] // HEAD, wk.shape[1] // HEAD
        nq, no = wq.shape[1] // TILE, d // TILE
        strips = heads * rows // STRIP
        dma = lambda n: pltpu.SemaphoreType.DMA((n,))
        vm = pltpu.VMEM
        tokens = 4 * rows
        return pl.pallas_call(
            _layer,
            out_shape=pltpu.VMEM((rows, d), BF16),
            in_specs=[pl.BlockSpec(memory_space=pl.ANY)] * 7,
            out_specs=pl.BlockSpec(memory_space=pltpu.VMEM),
            scratch_shapes=[
                vm((nq, d, TILE), BF16), vm((d, 2 * kv * HEAD), BF16), vm((no, heads * HEAD, TILE), BF16),
                vm((4, rows // 16, 16, d), BF16), vm((rows, d), BF16), vm((d // 128, 128), BF16), vm((d // 128, 128), F32), vm((tokens, HEAD), F32), vm((2, rows, HEAD), F32),
                vm((4, heads, rows, HEAD), BF16), vm((4, kv, rows, HEAD), BF16), vm((4, kv, HEAD + 16, rows), BF16),
                vm((strips, STRIP), F32), vm((strips * (HEAD + 16), STRIP), F32), vm((rows, STRIP), jnp.int32), vm((rows, heads * HEAD), BF16),
                vm((no // 2, rows, TILE), BF16), vm((no, rows, TILE), BF16), vm((no, rows, TILE), BF16), vm((no // 2, 2, rows, TILE), BF16),
                vm((no, rows, TILE), BF16),
                dma(7), dma(2), dma(1), dma(4), dma(2), dma(no // 2), dma(no // 2),
            ],
            compiler_params=pltpu.CompilerParams(collective_id=0, has_side_effects=True, vmem_limit_bytes=247 * 2**18),
            cost_estimate=pl.CostEstimate(flops=33 * 10**9, bytes_accessed=34 * 2**20, transcendentals=8 * 2**20),
            name="layer",
        )(x.reshape(rows // 16, 16, d), gain.reshape(d // 128, 128), jnp.asarray(_table(tokens)), wq, wk, wv, wo)

    tokens, columns = P(("dp", "tp"), None), P(None, "tp")
    return jax.shard_map(
        step,
        mesh=mesh,
        in_specs=(tokens, P(None), columns, columns, columns, P("tp", None)),
        out_specs=tokens,
        check_vma=False,
    )
```

```python
import functools

import jax
import jax.numpy as jnp
import numpy as np
from jax import lax
from jax.experimental import pallas as pl
from jax.experimental.pallas import tpu as pltpu
from jax.sharding import PartitionSpec as P

HEAD = 128
THETA = 10000
LOWEST = float(np.finfo(np.float32).min)
LOG2E = 1.4426950408889634
TILE = 512
STRIP = 512
F32, BF16 = jnp.float32, jnp.bfloat16


def _dot(a, b, ca=1, cb=0):
    return lax.dot_general(a, b, (((ca,), (cb,)), ((), ())), preferred_element_type=F32)


def _layer(x_hbm, gain_hbm, tab_hbm, wq_hbm, wk_hbm, wv_hbm, wo_hbm, y,
           wq, wkv, wo, xs, a, gain, gain_w, tab, rope, q, k, vt, top, mix, gap, seen, pp_out, pp_in, rs_out, rs_in, fin_in,
           ld, own_r, xs_s, ag_r, rl_r, pp_r, rs_r):
    me = lax.axis_index("tp")
    chip, core = me // 2, me % 2
    mate, peer = chip * 2 + 1 - core, (me + 2) % 4
    base, far = chip * 2, 2 - chip * 2
    rows = a.shape[0]
    d = a.shape[1]
    nq, no = wq.shape[0], wo.shape[0]
    heads, kv = q.shape[1], k.shape[1]
    group = heads // kv
    per = STRIP // rows
    half = no // 2
    hu = xs.shape[1] // 2

    def fin_out(n):
        return wq.at[1, pl.ds(pl.multiple_of(n * rows, rows), rows)]

    def send(src, dst, s, r, to):
        return pltpu.make_async_remote_copy(src, dst, s, r, device_id={"tp": to}, device_id_type=pl.DeviceIdType.MESH)

    wo_ld, pp_s, fin_s, rs_s, fin_r = ld.at[0], ld.at[1], ld.at[2], (ld.at[3], ld.at[4]), own_r.at[0]

    def all_of(ref, sem):
        return pltpu.make_async_copy(ref, ref, sem)

    def local_x(n):
        h = core if n < 2 else 1 - core
        at = pl.ds(h * hu + (n == 1), (1, hu - 1, hu)[n])
        return pltpu.make_async_copy(x_hbm.at[at], xs.at[me, at], ld.at[n])

    def own(n):
        at = pl.ds((1 - core if n == 0 else core) * hu, hu)
        return send(x_hbm.at[at], xs.at[me, at], xs_s.at[0], own_r.at[n], mate)

    def gather(p):
        blk, at, n, m = ((0, 0, 1, 0), (0, 1, hu // 2 - 1, 0), (0, hu // 2, hu // 2, 1), (1, 0, 1, 2), (1, 1, hu // 2 - 1, 2), (1, hu // 2, hu // 2, 3))[p]
        at = xs.at[base + blk, pl.ds(core * hu + at, n)]
        return send(at, at, xs_s.at[0], ag_r.at[m], peer)

    def quarter(m):
        return xs.at[far + m // 2, pl.ds(core * hu + m % 2 * (hu // 2), hu // 2)]

    def relay(m):
        return send(quarter(m), quarter(m), xs_s.at[0], rl_r.at[m // 2], mate)

    def relays(ms):
        for m in ms:
            all_of(quarter(m), ag_r.at[m]).wait()
            relay(m).start()

    def weights_q(n):
        return pltpu.make_async_copy(wq_hbm.at[:, pl.ds(pl.multiple_of(n * TILE, TILE), TILE)], wq.at[n], ld.at[6])

    def weights_o(n):
        return pltpu.make_async_copy(wo_hbm.at[:, pl.ds(pl.multiple_of(n * TILE, TILE), TILE)], wo.at[n], wo_ld)

    wide = kv * HEAD
    small = [
        pltpu.make_async_copy(gain_hbm, gain, ld.at[3]),
        pltpu.make_async_copy(tab_hbm, tab, ld.at[4]),
        pltpu.make_async_copy(wk_hbm, wkv.at[:, pl.ds(0, wide)], ld.at[5]),
        pltpu.make_async_copy(wv_hbm, wkv.at[:, pl.ds(wide, wide)], ld.at[5]),
    ]

    def norm(blk):
        step = 32
        units = step // xs.shape[2]

        def some(i, _):
            at = (blk, pl.ds(i * units, units))
            total = jnp.zeros((step, 128), F32)
            for c in range(0, d, 128):
                w = xs[(*at, slice(None), pl.ds(c, 128))].reshape(step, 128).astype(F32)
                total = total + w * w
            scale = lax.rsqrt(jnp.sum(total, axis=1, keepdims=True) * (1 / d) + 1e-6)
            for c in range(0, d, 128):
                w = xs[(*at, slice(None), pl.ds(c, 128))].reshape(step, 128).astype(F32)
                a[pl.ds(pl.multiple_of(i * step, step), step), pl.ds(c, 128)] = (w * scale * gain_w[pl.ds(c // 128, 1), :]).astype(BF16)
            return 0

        lax.fori_loop(0, rows // step, some, 0)

    def turned(t):
        t = t.astype(BF16).astype(F32)
        return (t * rope[0] + pltpu.roll(t, HEAD // 2, 1) * rope[1]).astype(BF16)

    def project(blk, loading):
        t = tab[pl.ds(pl.multiple_of(blk * rows, rows), rows), :]
        r = pltpu.roll(t, HEAD // 2, 1)
        first = lax.broadcasted_iota(jnp.int32, t.shape, 1) < HEAD // 2
        rope[0] = jnp.where(first, t, r)
        rope[1] = jnp.where(first, -r, t)
        if loading:
            all_of(wkv, ld.at[5]).wait()
        got = _dot(a[...], wkv[...])
        for i in range(kv):
            k[blk, i] = turned(got[:, i * HEAD : (i + 1) * HEAD])
            vt[blk, i, :HEAD, :] = got[:, wide + i * HEAD : wide + (i + 1) * HEAD].T.astype(BF16)

        if loading:
            all_of(wq, ld.at[6]).wait()

        def some(n, _):
            got = _dot(a[...], wq[n])
            for i in range(TILE // HEAD):
                q[blk, n * (TILE // HEAD) + i] = turned(got[:, i * HEAD : (i + 1) * HEAD])
            return 0

        lax.fori_loop(0, nq, some, 0)

    def attend(blk):
        e = HEAD**-0.5 * LOG2E
        deep = vt.shape[2]
        pieces = [(i, i * group + n) for i in range(kv) for n in range(0, group, per)]
        top[...] = jnp.full(top.shape, LOWEST, F32)
        mix[...] = jnp.zeros(mix.shape, F32)

        def block(j, masked):
            scores = [_dot(k[j, i], q[blk, pl.ds(n, per)].reshape(STRIP, HEAD), 1, 1) for i, n in pieces]
            weights, keeps = [], []
            for p, s in enumerate(scores):
                if masked:
                    s = jnp.where(gap[...] >= 0, s, LOWEST)
                old = top[p : p + 1, :]
                new = jnp.maximum(old, s.max(axis=0, keepdims=True))
                top[p : p + 1, :] = new
                weights.append(jnp.exp2((s - new) * e).astype(BF16))
                keeps.append(jnp.exp2((old - new) * e))
            for p, (w, keep) in enumerate(zip(weights, keeps)):
                at = pl.ds(p * deep, deep)
                mix[at, :] = mix[at, :] * keep + _dot(vt[j, pieces[p][0]], w)

        lax.fori_loop(0, blk, lambda j, _: (block(j, False), 0)[1], 0)
        block(blk, True)
        for p, (i, n) in enumerate(pieces):
            got = mix[p * deep : p * deep + HEAD, :] * (1 / mix[p * deep + HEAD : p * deep + HEAD + 1, :])
            for m in range(per):
                seen[:, (n + m) * HEAD : (n + m + 1) * HEAD] = got[:, m * rows : (m + 1) * rows].T.astype(BF16)

    def out_part(n):
        return _dot(seen[...], wo[n])

    def pass_on(b, t):
        return send(pp_out.at[t], pp_in.at[b * half + t], pp_s, pp_r.at[t], mate)

    def scatter(b, t):
        return send(rs_out.at[b * half + t], rs_in.at[t, core], rs_s[b], rs_r.at[t], far + b)

    def give(b):
        def mates(t):
            pp_out[t] = out_part((1 - core) * half + t).astype(BF16)
            pass_on(b, t).start()

        def mine(t):
            got = out_part(core * half + t)
            pass_on(b, t).wait_recv()
            rs_out[b * half + t] = (got + pp_in[b * half + t].astype(F32)).astype(BF16)
            scatter(b, t).start()

        def both(t, _):
            mates(t + 1)
            mine(t)
            return 0

        if b:
            all_of(pp_out, pp_s).wait()
        mates(0)
        lax.fori_loop(0, half - 1, both, 0)
        mine(half - 1)

    def last(n):
        return send(fin_out(n), fin_in.at[n], fin_s, fin_r, mate)

    def place(i):
        return (i % 2) * half + i // 2

    def mates_rows(i, _):
        n = place(i)
        fin_out(n)[...] = out_part(n).astype(BF16)
        last(n).start()
        return 0

    def my_rows(t, _):
        for h in range(2):
            n = h * half + t
            got = out_part(n)
            mine = xs[me, :, :, pl.ds(pl.multiple_of(n * TILE, TILE), TILE)].reshape(rows, TILE).astype(F32)
            mix[h * rows : (h + 1) * rows, :] = mine + (got + fin_in[n].astype(F32))
        all_of(rs_in.at[t], rs_r.at[t]).wait()
        for h in range(2):
            at = pl.ds(pl.multiple_of((h * half + t) * TILE, TILE), TILE)
            y[:, at] = (mix[h * rows : (h + 1) * rows, :] + rs_in[t, h].astype(F32)).astype(BF16)
        return 0

    for c in range(0, d, d // 4):
        at = (core * hu, slice(None), pl.ds(c, d // 4))
        pltpu.make_async_copy(x_hbm.at[at], xs.at[(me, *at)], ld.at[0]).start()
    barrier = pltpu.get_barrier_semaphore()
    for to in (mate, peer, (mate + 2) % 4):
        pl.semaphore_signal(barrier, 1, device_id={"tp": to}, device_id_type=pl.DeviceIdType.MESH)
    for n in (1, 2):
        local_x(n).start()
    pl.semaphore_wait(barrier, 3)
    own(0).start()
    own(1).start()
    local_x(0).wait()

    @pl.when(core == 0)
    def _():
        gather(0).start()

    @pl.when(core == 1)
    def _():
        gather(3).start()

    for copy in small:
        copy.start()
    for n in range(nq):
        weights_q(n).start()
    local_x(1).wait()

    @pl.when(core == 0)
    def _():
        gather(1).start()
        gather(2).start()

    own(0).wait_recv()

    @pl.when(core == 0)
    def _():
        gather(3).start()

    @pl.when(core == 1)
    def _():
        for p in range(3):
            gather(p).start()

    gather(4).start()
    gather(5).start()

    gap[...] = lax.rem(lax.broadcasted_iota(jnp.int32, gap.shape, 1), rows) - lax.broadcasted_iota(jnp.int32, gap.shape, 0)
    vt[:, :, HEAD:, :] = jnp.ones((4, kv, vt.shape[2] - HEAD, rows), BF16)

    local_x(2).wait()
    small[0].wait()
    gain_w[...] = gain[...].astype(F32)
    norm(me)
    small[1].wait()
    project(me, True)
    for n in range(no):
        weights_o(n).start()
    own(1).wait_recv()
    norm(mate)
    project(mate, False)

    for b in range(2):
        relays(((0, 1), (3,))[b])
        all_of(xs.at[far + b, pl.ds((1 - core) * hu, hu)], rl_r.at[b]).wait()
        norm(far + b)
        project(far + b, False)
        attend(far + b)
        if b == 0:
            relays((2,))
            all_of(wo, wo_ld).wait()
        give(b)

    attend(mate)
    lax.fori_loop(0, no, mates_rows, 0)
    attend(me)

    all_of(xs.at[pl.ds(0, 3)], xs_s.at[0]).wait()
    all_of(pp_out, pp_s).wait()
    all_of(fin_in, fin_s).wait()
    all_of(pp_out, rs_s[0]).wait()
    all_of(fin_in, fin_r).wait()

    lax.fori_loop(0, half, my_rows, 0)

    all_of(pp_out, rs_s[1]).wait()


def _table(tokens):
    half = HEAD // 2
    angle = np.arange(tokens, dtype=np.float32)[:, None] * np.float32(THETA) ** (-np.arange(half, dtype=np.float32) / np.float32(half))
    angle = angle.astype(np.float64)
    return np.concatenate([np.cos(angle), np.sin(angle)], -1).astype(np.float32)


def solution(mesh):
    def step(x, gain, wq, wk, wv, wo):
        rows, d = x.shape
        heads, kv = wq.shape[1] // HEAD, wk.shape[1] // HEAD
        nq, no = wq.shape[1] // TILE, d // TILE
        strips = heads * rows // STRIP
        dma = lambda n: pltpu.SemaphoreType.DMA((n,))
        vm = pltpu.VMEM
        tokens = 4 * rows
        return pl.pallas_call(
            _layer,
            out_shape=pltpu.VMEM((rows, d), BF16),
            in_specs=[pl.BlockSpec(memory_space=pl.ANY)] * 7,
            out_specs=pl.BlockSpec(memory_space=pltpu.VMEM),
            scratch_shapes=[
                vm((nq, d, TILE), BF16), vm((d, 2 * kv * HEAD), BF16), vm((no, heads * HEAD, TILE), BF16),
                vm((4, rows // 16, 16, d), BF16), vm((rows, d), BF16), vm((d // 128, 128), BF16), vm((d // 128, 128), F32), vm((tokens, HEAD), F32), vm((2, rows, HEAD), F32),
                vm((4, heads, rows, HEAD), BF16), vm((4, kv, rows, HEAD), BF16), vm((4, kv, HEAD + 16, rows), BF16),
                vm((strips, STRIP), F32), vm((strips * (HEAD + 16), STRIP), F32), vm((rows, STRIP), jnp.int32), vm((rows, heads * HEAD), BF16),
                vm((no // 2, rows, TILE), BF16), vm((no, rows, TILE), BF16), vm((no, rows, TILE), BF16), vm((no // 2, 2, rows, TILE), BF16),
                vm((no, rows, TILE), BF16),
                dma(7), dma(2), dma(1), dma(4), dma(2), dma(no // 2), dma(no // 2),
            ],
            compiler_params=pltpu.CompilerParams(collective_id=0, has_side_effects=True, vmem_limit_bytes=247 * 2**18),
            cost_estimate=pl.CostEstimate(flops=33 * 10**9, bytes_accessed=34 * 2**20, transcendentals=8 * 2**20),
            name="layer",
        )(x.reshape(rows // 16, 16, d), gain.reshape(d // 128, 128), jnp.asarray(_table(tokens)), wq, wk, wv, wo)

    tokens, columns = P(("dp", "tp"), None), P(None, "tp")
    return jax.shard_map(
        step,
        mesh=mesh,
        in_specs=(tokens, P(None), columns, columns, columns, P("tp", None)),
        out_specs=tokens,
        check_vma=False,
    )
```

```python
import functools

import jax
import jax.numpy as jnp
import numpy as np
from jax import lax
from jax.experimental import pallas as pl
from jax.experimental.pallas import tpu as pltpu
from jax.sharding import PartitionSpec as P

HEAD = 128
THETA = 10000
LOWEST = float(np.finfo(np.float32).min)
LOG2E = 1.4426950408889634
TILE = 512
STRIP = 512
F32, BF16 = jnp.float32, jnp.bfloat16


def _dot(a, b, ca=1, cb=0):
    return lax.dot_general(a, b, (((ca,), (cb,)), ((), ())), preferred_element_type=F32)


def _layer(x_hbm, gain_hbm, tab_hbm, wq_hbm, wk_hbm, wv_hbm, wo_hbm, y,
           wq, wkv, wo, xs, a, gain, gain_w, tab, rope, q, k, vt, top, mix, gap, seen, pp_out, pp_in, rs_out, rs_in, fin_in,
           ld, own_r, xs_s, ag_r, rl_r, pp_r, rs_r):
    me = lax.axis_index("tp")
    chip, core = me // 2, me % 2
    mate, peer = chip * 2 + 1 - core, (me + 2) % 4
    base, far = chip * 2, 2 - chip * 2
    rows = a.shape[0]
    d = a.shape[1]
    nq, no = wq.shape[0], wo.shape[0]
    heads, kv = q.shape[1], k.shape[1]
    group = heads // kv
    per = STRIP // rows
    half = no // 2
    hu = xs.shape[1] // 2

    def fin_out(n):
        return wq.at[1, pl.ds(pl.multiple_of(n * rows, rows), rows)]

    def send(src, dst, s, r, to):
        return pltpu.make_async_remote_copy(src, dst, s, r, device_id={"tp": to}, device_id_type=pl.DeviceIdType.MESH)

    wo_ld, pp_s, fin_s, rs_s, fin_r = ld.at[0], ld.at[1], ld.at[2], (ld.at[3], ld.at[4]), own_r.at[0]

    def all_of(ref, sem):
        return pltpu.make_async_copy(ref, ref, sem)

    def local_x(n):
        h = core if n < 2 else 1 - core
        at = pl.ds(h * hu + (n == 1), (1, hu - 1, hu)[n])
        return pltpu.make_async_copy(x_hbm.at[at], xs.at[me, at], ld.at[n])

    def own(n):
        at = pl.ds((1 - core if n == 0 else core) * hu, hu)
        return send(x_hbm.at[at], xs.at[me, at], xs_s.at[0], own_r.at[n], mate)

    def gather(p):
        blk, at, n, m = ((0, 0, 1, 0), (0, 1, hu // 2 - 1, 0), (0, hu // 2, hu // 2, 1), (1, 0, 1, 2), (1, 1, hu // 2 - 1, 2), (1, hu // 2, hu // 2, 3))[p]
        at = xs.at[base + blk, pl.ds(core * hu + at, n)]
        return send(at, at, xs_s.at[0], ag_r.at[m], peer)

    def quarter(m):
        return xs.at[far + m // 2, pl.ds(core * hu + m % 2 * (hu // 2), hu // 2)]

    def relay(m):
        return send(quarter(m), quarter(m), xs_s.at[0], rl_r.at[m // 2], mate)

    def relays(ms):
        for m in ms:
            all_of(quarter(m), ag_r.at[m]).wait()
            relay(m).start()

    def weights_q(n):
        return pltpu.make_async_copy(wq_hbm.at[:, pl.ds(pl.multiple_of(n * TILE, TILE), TILE)], wq.at[n], ld.at[6])

    def weights_o(n):
        return pltpu.make_async_copy(wo_hbm.at[:, pl.ds(pl.multiple_of(n * TILE, TILE), TILE)], wo.at[n], wo_ld)

    wide = kv * HEAD
    small = [
        pltpu.make_async_copy(gain_hbm, gain, ld.at[3]),
        pltpu.make_async_copy(tab_hbm, tab, ld.at[4]),
        pltpu.make_async_copy(wk_hbm, wkv.at[:, pl.ds(0, wide)], ld.at[5]),
        pltpu.make_async_copy(wv_hbm, wkv.at[:, pl.ds(wide, wide)], ld.at[5]),
    ]

    def norm(blk):
        step = 32
        units = step // xs.shape[2]

        def some(i, _):
            at = (blk, pl.ds(i * units, units))
            total = jnp.zeros((step, 128), F32)
            for c in range(0, d, 128):
                w = xs[(*at, slice(None), pl.ds(c, 128))].reshape(step, 128).astype(F32)
                total = total + w * w
            scale = lax.rsqrt(jnp.sum(total, axis=1, keepdims=True) * (1 / d) + 1e-6)
            for c in range(0, d, 128):
                w = xs[(*at, slice(None), pl.ds(c, 128))].reshape(step, 128).astype(F32)
                a[pl.ds(pl.multiple_of(i * step, step), step), pl.ds(c, 128)] = (w * scale * gain_w[pl.ds(c // 128, 1), :]).astype(BF16)
            return 0

        lax.fori_loop(0, rows // step, some, 0)

    def turned(t):
        t = t.astype(BF16).astype(F32)
        return (t * rope[0] + pltpu.roll(t, HEAD // 2, 1) * rope[1]).astype(BF16)

    def project(blk, loading):
        t = tab[pl.ds(pl.multiple_of(blk * rows, rows), rows), :]
        r = pltpu.roll(t, HEAD // 2, 1)
        first = lax.broadcasted_iota(jnp.int32, t.shape, 1) < HEAD // 2
        rope[0] = jnp.where(first, t, r)
        rope[1] = jnp.where(first, -r, t)
        if loading:
            all_of(wkv, ld.at[5]).wait()
        got = _dot(a[...], wkv[...])
        for i in range(kv):
            k[blk, i] = turned(got[:, i * HEAD : (i + 1) * HEAD])
            vt[blk, i, :HEAD, :] = got[:, wide + i * HEAD : wide + (i + 1) * HEAD].T.astype(BF16)

        if loading:
            all_of(wq, ld.at[6]).wait()

        def some(n, _):
            got = _dot(a[...], wq[n])
            for i in range(TILE // HEAD):
                q[blk, n * (TILE // HEAD) + i] = turned(got[:, i * HEAD : (i + 1) * HEAD])
            return 0

        lax.fori_loop(0, nq, some, 0)

    def attend(blk):
        e = HEAD**-0.5 * LOG2E
        deep = vt.shape[2]
        pieces = [(i, i * group + n) for i in range(kv) for n in range(0, group, per)]
        top[...] = jnp.full(top.shape, LOWEST, F32)
        mix[...] = jnp.zeros(mix.shape, F32)

        def block(j, masked):
            scores = [_dot(k[j, i], q[blk, pl.ds(n, per)].reshape(STRIP, HEAD), 1, 1) for i, n in pieces]
            weights, keeps = [], []
            for p, s in enumerate(scores):
                if masked:
                    s = jnp.where(gap[...] >= 0, s, LOWEST)
                old = top[p : p + 1, :]
                new = jnp.maximum(old, s.max(axis=0, keepdims=True))
                top[p : p + 1, :] = new
                weights.append(jnp.exp2((s - new) * e).astype(BF16))
                keeps.append(jnp.exp2((old - new) * e))
            for p, (w, keep) in enumerate(zip(weights, keeps)):
                at = pl.ds(p * deep, deep)
                mix[at, :] = mix[at, :] * keep + _dot(vt[j, pieces[p][0]], w)

        lax.fori_loop(0, blk, lambda j, _: (block(j, False), 0)[1], 0)
        block(blk, True)
        for p, (i, n) in enumerate(pieces):
            got = mix[p * deep : p * deep + HEAD, :] * (1 / mix[p * deep + HEAD : p * deep + HEAD + 1, :])
            for m in range(per):
                seen[:, (n + m) * HEAD : (n + m + 1) * HEAD] = got[:, m * rows : (m + 1) * rows].T.astype(BF16)

    def out_part(n):
        return _dot(seen[...], wo[n])

    def pass_on(b, t):
        return send(pp_out.at[t], pp_in.at[b * half + t], pp_s, pp_r.at[t], mate)

    def scatter(b, t):
        return send(rs_out.at[b * half + t], rs_in.at[t, core], rs_s[b], rs_r.at[t], far + b)

    def give(b):
        def mates(t):
            pp_out[t] = out_part((1 - core) * half + t).astype(BF16)
            pass_on(b, t).start()

        def mine(t):
            got = out_part(core * half + t)
            pass_on(b, t).wait_recv()
            rs_out[b * half + t] = (got + pp_in[b * half + t].astype(F32)).astype(BF16)
            scatter(b, t).start()

        def both(t, _):
            mates(t + 1)
            mine(t)
            return 0

        if b:
            all_of(pp_out, pp_s).wait()
        mates(0)
        lax.fori_loop(0, half - 1, both, 0)
        mine(half - 1)

    def last(n):
        return send(fin_out(n), fin_in.at[n], fin_s, fin_r, mate)

    def place(i):
        return (i % 2) * half + i // 2

    def mates_rows(i, _):
        n = place(i)
        fin_out(n)[...] = out_part(n).astype(BF16)
        last(n).start()
        return 0

    def my_rows(t, _):
        for h in range(2):
            n = h * half + t
            got = out_part(n)
            mine = xs[me, :, :, pl.ds(pl.multiple_of(n * TILE, TILE), TILE)].reshape(rows, TILE).astype(F32)
            mix[h * rows : (h + 1) * rows, :] = mine + (got + fin_in[n].astype(F32))
        all_of(rs_in.at[t], rs_r.at[t]).wait()
        for h in range(2):
            at = pl.ds(pl.multiple_of((h * half + t) * TILE, TILE), TILE)
            y[:, at] = (mix[h * rows : (h + 1) * rows, :] + rs_in[t, h].astype(F32)).astype(BF16)
        return 0

    for c in range(0, d, d // 4):
        at = (core * hu, slice(None), pl.ds(c, d // 4))
        pltpu.make_async_copy(x_hbm.at[at], xs.at[(me, *at)], ld.at[0]).start()
    barrier = pltpu.get_barrier_semaphore()
    for to in (mate, peer, (mate + 2) % 4):
        pl.semaphore_signal(barrier, 1, device_id={"tp": to}, device_id_type=pl.DeviceIdType.MESH)
    for n in (1, 2):
        local_x(n).start()
    pl.semaphore_wait(barrier, 3)
    own(0).start()
    own(1).start()
    first = pl.ds(core * hu, 1)
    send(x_hbm.at[first], xs.at[me, first], xs_s.at[0], ag_r.at[2 * core], peer).start()
    all_of(xs.at[me, first], ld.at[0]).wait()
    for copy in small:
        copy.start()
    for n in range(nq):
        weights_q(n).start()
    local_x(1).wait()

    @pl.when(core == 0)
    def _():
        gather(1).start()
        gather(2).start()

    own(0).wait_recv()

    @pl.when(core == 0)
    def _():
        gather(3).start()

    @pl.when(core == 1)
    def _():
        for p in range(3):
            gather(p).start()

    gather(4).start()
    gather(5).start()

    gap[...] = lax.rem(lax.broadcasted_iota(jnp.int32, gap.shape, 1), rows) - lax.broadcasted_iota(jnp.int32, gap.shape, 0)
    vt[:, :, HEAD:, :] = jnp.ones((4, kv, vt.shape[2] - HEAD, rows), BF16)

    local_x(2).wait()
    small[0].wait()
    gain_w[...] = gain[...].astype(F32)
    norm(me)
    small[1].wait()
    project(me, True)
    for n in range(no):
        weights_o(n).start()
    own(1).wait_recv()
    norm(mate)
    project(mate, False)

    for b in range(2):
        relays(((0, 1), (3,))[b])
        all_of(xs.at[far + b, pl.ds((1 - core) * hu, hu)], rl_r.at[b]).wait()
        norm(far + b)
        project(far + b, False)
        attend(far + b)
        if b == 0:
            relays((2,))
            all_of(wo, wo_ld).wait()
        give(b)

    attend(mate)
    lax.fori_loop(0, no, mates_rows, 0)
    attend(me)

    all_of(xs.at[pl.ds(0, 3)], xs_s.at[0]).wait()
    all_of(pp_out, pp_s).wait()
    all_of(fin_in, fin_s).wait()
    all_of(pp_out, rs_s[0]).wait()
    all_of(fin_in, fin_r).wait()

    lax.fori_loop(0, half, my_rows, 0)

    all_of(pp_out, rs_s[1]).wait()


def _table(tokens):
    half = HEAD // 2
    angle = np.arange(tokens, dtype=np.float32)[:, None] * np.float32(THETA) ** (-np.arange(half, dtype=np.float32) / np.float32(half))
    angle = angle.astype(np.float64)
    return np.concatenate([np.cos(angle), np.sin(angle)], -1).astype(np.float32)


def solution(mesh):
    def step(x, gain, wq, wk, wv, wo):
        rows, d = x.shape
        heads, kv = wq.shape[1] // HEAD, wk.shape[1] // HEAD
        nq, no = wq.shape[1] // TILE, d // TILE
        strips = heads * rows // STRIP
        dma = lambda n: pltpu.SemaphoreType.DMA((n,))
        vm = pltpu.VMEM
        tokens = 4 * rows
        return pl.pallas_call(
            _layer,
            out_shape=pltpu.VMEM((rows, d), BF16),
            in_specs=[pl.BlockSpec(memory_space=pl.ANY)] * 7,
            out_specs=pl.BlockSpec(memory_space=pltpu.VMEM),
            scratch_shapes=[
                vm((nq, d, TILE), BF16), vm((d, 2 * kv * HEAD), BF16), vm((no, heads * HEAD, TILE), BF16),
                vm((4, rows // 16, 16, d), BF16), vm((rows, d), BF16), vm((d // 128, 128), BF16), vm((d // 128, 128), F32), vm((tokens, HEAD), F32), vm((2, rows, HEAD), F32),
                vm((4, heads, rows, HEAD), BF16), vm((4, kv, rows, HEAD), BF16), vm((4, kv, HEAD + 16, rows), BF16),
                vm((strips, STRIP), F32), vm((strips * (HEAD + 16), STRIP), F32), vm((rows, STRIP), jnp.int32), vm((rows, heads * HEAD), BF16),
                vm((no // 2, rows, TILE), BF16), vm((no, rows, TILE), BF16), vm((no, rows, TILE), BF16), vm((no // 2, 2, rows, TILE), BF16),
                vm((no, rows, TILE), BF16),
                dma(7), dma(2), dma(1), dma(4), dma(2), dma(no // 2), dma(no // 2),
            ],
            compiler_params=pltpu.CompilerParams(collective_id=0, has_side_effects=True, vmem_limit_bytes=247 * 2**18),
            cost_estimate=pl.CostEstimate(flops=33 * 10**9, bytes_accessed=34 * 2**20, transcendentals=8 * 2**20),
            name="layer",
        )(x.reshape(rows // 16, 16, d), gain.reshape(d // 128, 128), jnp.asarray(_table(tokens)), wq, wk, wv, wo)

    tokens, columns = P(("dp", "tp"), None), P(None, "tp")
    return jax.shard_map(
        step,
        mesh=mesh,
        in_specs=(tokens, P(None), columns, columns, columns, P("tp", None)),
        out_specs=tokens,
        check_vma=False,
    )
```

```python
import functools

import jax
import jax.numpy as jnp
import numpy as np
from jax import lax
from jax.experimental import pallas as pl
from jax.experimental.pallas import tpu as pltpu
from jax.sharding import PartitionSpec as P

HEAD = 128
THETA = 10000
LOWEST = float(np.finfo(np.float32).min)
LOG2E = 1.4426950408889634
TILE = 512
STRIP = 512
F32, BF16 = jnp.float32, jnp.bfloat16


def _dot(a, b, ca=1, cb=0):
    return lax.dot_general(a, b, (((ca,), (cb,)), ((), ())), preferred_element_type=F32)


def _layer(x_hbm, gain_hbm, tab_hbm, wq_hbm, wk_hbm, wv_hbm, wo_hbm, y,
           wq, wkv, wo, xs, a, gain, gain_w, tab, rope, q, k, vt, top, mix, gap, seen, pp_out, pp_in, rs_out, rs_in, fin_in,
           ld, own_r, xs_s, ag_r, rl_r, pp_r, rs_r):
    me = lax.axis_index("tp")
    chip, core = me // 2, me % 2
    mate, peer = chip * 2 + 1 - core, (me + 2) % 4
    base, far = chip * 2, 2 - chip * 2
    rows = a.shape[0]
    d = a.shape[1]
    nq, no = wq.shape[0], wo.shape[0]
    heads, kv = q.shape[1], k.shape[1]
    group = heads // kv
    per = STRIP // rows
    half = no // 2
    hu = xs.shape[1] // 2

    def fin_out(n):
        return wq.at[1, pl.ds(pl.multiple_of(n * rows, rows), rows)]

    def send(src, dst, s, r, to):
        return pltpu.make_async_remote_copy(src, dst, s, r, device_id={"tp": to}, device_id_type=pl.DeviceIdType.MESH)

    wo_ld, pp_s, fin_s, rs_s, fin_r = ld.at[0], ld.at[1], ld.at[2], (ld.at[3], ld.at[4]), own_r.at[0]

    def all_of(ref, sem):
        return pltpu.make_async_copy(ref, ref, sem)

    def local_x(n):
        h = core if n < 2 else 1 - core
        at = pl.ds(h * hu + (n == 1), (1, hu - 1, hu)[n])
        return pltpu.make_async_copy(x_hbm.at[at], xs.at[me, at], ld.at[n])

    def own(n):
        at = pl.ds((1 - core if n == 0 else core) * hu, hu)
        return send(x_hbm.at[at], xs.at[me, at], xs_s.at[0], own_r.at[n], mate)

    def gather(p):
        blk, at, n, m = ((0, 0, 1, 0), (0, 1, hu // 2 - 1, 0), (0, hu // 2, hu // 2, 1), (1, 0, 1, 2), (1, 1, hu // 2 - 1, 2), (1, hu // 2, hu // 2, 3))[p]
        at = xs.at[base + blk, pl.ds(core * hu + at, n)]
        return send(at, at, xs_s.at[0], ag_r.at[m], peer)

    def quarter(m):
        return xs.at[far + m // 2, pl.ds(core * hu + m % 2 * (hu // 2), hu // 2)]

    def relay(m):
        return send(quarter(m), quarter(m), xs_s.at[0], rl_r.at[m // 2], mate)

    def relays(ms):
        for m in ms:
            all_of(quarter(m), ag_r.at[m]).wait()
            relay(m).start()

    def weights_q(n):
        return pltpu.make_async_copy(wq_hbm.at[:, pl.ds(pl.multiple_of(n * TILE, TILE), TILE)], wq.at[n], ld.at[5])

    def weights_o(n):
        return pltpu.make_async_copy(wo_hbm.at[:, pl.ds(pl.multiple_of(n * TILE, TILE), TILE)], wo.at[n], wo_ld)

    wide = kv * HEAD
    small = [
        pltpu.make_async_copy(gain_hbm, gain, ld.at[3]),
        pltpu.make_async_copy(tab_hbm, tab, ld.at[0]),
        pltpu.make_async_copy(wk_hbm, wkv.at[:, pl.ds(0, wide)], ld.at[4]),
        pltpu.make_async_copy(wv_hbm, wkv.at[:, pl.ds(wide, wide)], ld.at[4]),
    ]

    def norm(blk):
        step = 32
        units = step // xs.shape[2]

        def some(i, _):
            at = (blk, pl.ds(i * units, units))
            total = jnp.zeros((step, 128), F32)
            for c in range(0, d, 128):
                w = xs[(*at, slice(None), pl.ds(c, 128))].reshape(step, 128).astype(F32)
                total = total + w * w
            scale = lax.rsqrt(jnp.sum(total, axis=1, keepdims=True) * (1 / d) + 1e-6)
            for c in range(0, d, 128):
                w = xs[(*at, slice(None), pl.ds(c, 128))].reshape(step, 128).astype(F32)
                a[pl.ds(pl.multiple_of(i * step, step), step), pl.ds(c, 128)] = (w * scale * gain_w[pl.ds(c // 128, 1), :]).astype(BF16)
            return 0

        lax.fori_loop(0, rows // step, some, 0)

    def turned(t):
        t = t.astype(BF16).astype(F32)
        return (t * rope[0] + pltpu.roll(t, HEAD // 2, 1) * rope[1]).astype(BF16)

    def project(blk, loading):
        t = tab[pl.ds(pl.multiple_of(blk * rows, rows), rows), :]
        r = pltpu.roll(t, HEAD // 2, 1)
        first = lax.broadcasted_iota(jnp.int32, t.shape, 1) < HEAD // 2
        rope[0] = jnp.where(first, t, r)
        rope[1] = jnp.where(first, -r, t)
        if loading:
            all_of(wkv, ld.at[4]).wait()
        got = _dot(a[...], wkv[...])
        for i in range(kv):
            k[blk, i] = turned(got[:, i * HEAD : (i + 1) * HEAD])
            vt[blk, i, :HEAD, :] = got[:, wide + i * HEAD : wide + (i + 1) * HEAD].T.astype(BF16)

        if loading:
            all_of(wq, ld.at[5]).wait()

        def some(n, _):
            got = _dot(a[...], wq[n])
            for i in range(TILE // HEAD):
                q[blk, n * (TILE // HEAD) + i] = turned(got[:, i * HEAD : (i + 1) * HEAD])
            return 0

        lax.fori_loop(0, nq, some, 0)

    def attend(blk):
        e = HEAD**-0.5 * LOG2E
        deep = vt.shape[2]
        pieces = [(i, i * group + n) for i in range(kv) for n in range(0, group, per)]
        top[...] = jnp.full(top.shape, LOWEST, F32)
        mix[...] = jnp.zeros(mix.shape, F32)

        def block(j, masked):
            scores = [_dot(k[j, i], q[blk, pl.ds(n, per)].reshape(STRIP, HEAD), 1, 1) for i, n in pieces]
            weights, keeps = [], []
            for p, s in enumerate(scores):
                if masked:
                    s = jnp.where(gap[...] >= 0, s, LOWEST)
                old = top[p : p + 1, :]
                new = jnp.maximum(old, s.max(axis=0, keepdims=True))
                top[p : p + 1, :] = new
                weights.append(jnp.exp2((s - new) * e).astype(BF16))
                keeps.append(jnp.exp2((old - new) * e))
            for p, (w, keep) in enumerate(zip(weights, keeps)):
                at = pl.ds(p * deep, deep)
                mix[at, :] = mix[at, :] * keep + _dot(vt[j, pieces[p][0]], w)

        lax.fori_loop(0, blk, lambda j, _: (block(j, False), 0)[1], 0)
        block(blk, True)
        for p, (i, n) in enumerate(pieces):
            got = mix[p * deep : p * deep + HEAD, :] * (1 / mix[p * deep + HEAD : p * deep + HEAD + 1, :])
            for m in range(per):
                seen[:, (n + m) * HEAD : (n + m + 1) * HEAD] = got[:, m * rows : (m + 1) * rows].T.astype(BF16)

    def out_part(n):
        return _dot(seen[...], wo[n])

    def pass_on(b, t):
        return send(pp_out.at[t], pp_in.at[b * half + t], pp_s, pp_r.at[t], mate)

    def scatter(b, t):
        return send(rs_out.at[b * half + t], rs_in.at[t, core], rs_s[b], rs_r.at[t // (half - 1)], far + b)

    def give(b):
        def mates(t):
            pp_out[t] = out_part((1 - core) * half + t).astype(BF16)
            pass_on(b, t).start()

        def mine(t):
            got = out_part(core * half + t)
            pass_on(b, t).wait_recv()
            rs_out[b * half + t] = (got + pp_in[b * half + t].astype(F32)).astype(BF16)
            scatter(b, t).start()

        def both(t, _):
            mates(t + 1)
            mine(t)
            return 0

        if b:
            all_of(pp_out, pp_s).wait()
        mates(0)
        lax.fori_loop(0, half - 1, both, 0)
        mine(half - 1)

    def last(n):
        return send(fin_out(n), fin_in.at[n], fin_s, fin_r, mate)

    def place(i):
        return (i % 2) * half + i // 2

    def mates_rows(i, _):
        n = place(i)
        fin_out(n)[...] = out_part(n).astype(BF16)
        last(n).start()
        return 0

    def my_rows(t, _):
        for h in range(2):
            n = h * half + t
            got = out_part(n)
            mine = xs[me, :, :, pl.ds(pl.multiple_of(n * TILE, TILE), TILE)].reshape(rows, TILE).astype(F32)
            mix[h * rows : (h + 1) * rows, :] = mine + (got + fin_in[n].astype(F32))
        @pl.when(t == 0)
        def _():
            all_of(rs_in.at[pl.ds(0, half - 1)], rs_r.at[0]).wait()

        @pl.when(t == half - 1)
        def _():
            all_of(rs_in.at[half - 1], rs_r.at[1]).wait()

        for h in range(2):
            at = pl.ds(pl.multiple_of((h * half + t) * TILE, TILE), TILE)
            y[:, at] = (mix[h * rows : (h + 1) * rows, :] + rs_in[t, h].astype(F32)).astype(BF16)
        return 0

    for c in range(0, d, d // 4):
        at = (core * hu, slice(None), pl.ds(c, d // 4))
        pltpu.make_async_copy(x_hbm.at[at], xs.at[(me, *at)], ld.at[0]).start()
    barrier = pltpu.get_barrier_semaphore()
    for to in (mate, peer, (mate + 2) % 4):
        pl.semaphore_signal(barrier, 1, device_id={"tp": to}, device_id_type=pl.DeviceIdType.MESH)
    for n in (1, 2):
        local_x(n).start()
    pl.semaphore_wait(barrier, 3)
    own(0).start()
    own(1).start()
    first = pl.ds(core * hu, 1)
    send(x_hbm.at[first], xs.at[me, first], xs_s.at[0], ag_r.at[2 * core], peer).start()
    all_of(xs.at[me, first], ld.at[0]).wait()
    for copy in small:
        copy.start()
    for n in range(nq):
        weights_q(n).start()
    local_x(1).wait()

    @pl.when(core == 0)
    def _():
        gather(1).start()
        gather(2).start()

    gap[...] = lax.rem(lax.broadcasted_iota(jnp.int32, gap.shape, 1), rows) - lax.broadcasted_iota(jnp.int32, gap.shape, 0)
    vt[:, :, HEAD:, :] = jnp.ones((4, kv, vt.shape[2] - HEAD, rows), BF16)

    local_x(2).wait()
    small[0].wait()
    gain_w[...] = gain[...].astype(F32)
    norm(me)

    own(0).wait_recv()

    @pl.when(core == 0)
    def _():
        gather(3).start()

    @pl.when(core == 1)
    def _():
        for p in range(3):
            gather(p).start()

    gather(4).start()
    gather(5).start()

    small[1].wait()
    project(me, True)
    for n in range(no):
        weights_o(n).start()
    own(1).wait_recv()
    norm(mate)
    project(mate, False)

    for b in range(2):
        relays(((0, 1), (3,))[b])
        all_of(xs.at[far + b, pl.ds((1 - core) * hu, hu)], rl_r.at[b]).wait()
        norm(far + b)
        project(far + b, False)
        attend(far + b)
        if b == 0:
            relays((2,))
            all_of(wo, wo_ld).wait()
        give(b)

    attend(mate)
    lax.fori_loop(0, no, mates_rows, 0)
    attend(me)

    all_of(xs.at[pl.ds(0, 3)], xs_s.at[0]).wait()
    all_of(pp_out, pp_s).wait()
    all_of(fin_in, fin_s).wait()
    all_of(pp_out, rs_s[0]).wait()
    all_of(fin_in, fin_r).wait()

    lax.fori_loop(0, half, my_rows, 0)

    all_of(pp_out, rs_s[1]).wait()


def _table(tokens):
    half = HEAD // 2
    angle = np.arange(tokens, dtype=np.float32)[:, None] * np.float32(THETA) ** (-np.arange(half, dtype=np.float32) / np.float32(half))
    angle = angle.astype(np.float64)
    return np.concatenate([np.cos(angle), np.sin(angle)], -1).astype(np.float32)


def solution(mesh):
    def step(x, gain, wq, wk, wv, wo):
        rows, d = x.shape
        heads, kv = wq.shape[1] // HEAD, wk.shape[1] // HEAD
        nq, no = wq.shape[1] // TILE, d // TILE
        strips = heads * rows // STRIP
        dma = lambda n: pltpu.SemaphoreType.DMA((n,))
        vm = pltpu.VMEM
        tokens = 4 * rows
        return pl.pallas_call(
            _layer,
            out_shape=pltpu.VMEM((rows, d), BF16),
            in_specs=[pl.BlockSpec(memory_space=pl.ANY)] * 7,
            out_specs=pl.BlockSpec(memory_space=pltpu.VMEM),
            scratch_shapes=[
                vm((nq, d, TILE), BF16), vm((d, 2 * kv * HEAD), BF16), vm((no, heads * HEAD, TILE), BF16),
                vm((4, rows // 16, 16, d), BF16), vm((rows, d), BF16), vm((d // 128, 128), BF16), vm((d // 128, 128), F32), vm((tokens, HEAD), F32), vm((2, rows, HEAD), F32),
                vm((4, heads, rows, HEAD), BF16), vm((4, kv, rows, HEAD), BF16), vm((4, kv, HEAD + 16, rows), BF16),
                vm((strips, STRIP), F32), vm((strips * (HEAD + 16), STRIP), F32), vm((rows, STRIP), jnp.int32), vm((rows, heads * HEAD), BF16),
                vm((no // 2, rows, TILE), BF16), vm((no, rows, TILE), BF16), vm((no, rows, TILE), BF16), vm((no // 2, 2, rows, TILE), BF16),
                vm((no, rows, TILE), BF16),
                dma(6), dma(2), dma(1), dma(4), dma(2), dma(no // 2), dma(2),
            ],
            compiler_params=pltpu.CompilerParams(collective_id=0, has_side_effects=True, vmem_limit_bytes=247 * 2**18),
            cost_estimate=pl.CostEstimate(flops=33 * 10**9, bytes_accessed=34 * 2**20, transcendentals=8 * 2**20),
            name="layer",
        )(x.reshape(rows // 16, 16, d), gain.reshape(d // 128, 128), jnp.asarray(_table(tokens)), wq, wk, wv, wo)

    tokens, columns = P(("dp", "tp"), None), P(None, "tp")
    return jax.shard_map(
        step,
        mesh=mesh,
        in_specs=(tokens, P(None), columns, columns, columns, P("tp", None)),
        out_specs=tokens,
        check_vma=False,
    )
```

```python
import functools

import jax
import jax.numpy as jnp
import numpy as np
from jax import lax
from jax.experimental import pallas as pl
from jax.experimental.pallas import tpu as pltpu
from jax.sharding import PartitionSpec as P

HEAD = 128
THETA = 10000
LOWEST = float(np.finfo(np.float32).min)
LOG2E = 1.4426950408889634
TILE = 512
STRIP = 512
F32, BF16 = jnp.float32, jnp.bfloat16


def _dot(a, b, ca=1, cb=0):
    return lax.dot_general(a, b, (((ca,), (cb,)), ((), ())), preferred_element_type=F32)


def _layer(x_hbm, gain_hbm, tab_hbm, wq_hbm, wk_hbm, wv_hbm, wo_hbm, y,
           wq, wkv, wo, xs, a, gain, gain_w, tab, rope, q, k, vt, top, mix, gap, seen, pp_out, pp_in, rs_out, rs_in, fin_in,
           ld, own_r, xs_s, ag_r, rl_r, pp_r, rs_r):
    me = lax.axis_index("tp")
    chip, core = me // 2, me % 2
    mate, peer = chip * 2 + 1 - core, (me + 2) % 4
    base, far = chip * 2, 2 - chip * 2
    rows = a.shape[0]
    d = a.shape[1]
    nq, no = wq.shape[0], wo.shape[0]
    heads, kv = q.shape[1], k.shape[1]
    group = heads // kv
    per = STRIP // rows
    half = no // 2
    hu = xs.shape[1] // 2

    def fin_out(n):
        return wq.at[1, pl.ds(pl.multiple_of(n * rows, rows), rows)]

    def send(src, dst, s, r, to):
        return pltpu.make_async_remote_copy(src, dst, s, r, device_id={"tp": to}, device_id_type=pl.DeviceIdType.MESH)

    wo_ld, pp_s, fin_s, rs_s, fin_r = ld.at[0], ld.at[1], ld.at[2], (ld.at[3], ld.at[4]), own_r.at[0]

    def all_of(ref, sem):
        return pltpu.make_async_copy(ref, ref, sem)

    def local_x(n):
        h = core if n < 2 else 1 - core
        at = pl.ds(h * hu + (n == 1), (1, hu - 1, hu)[n])
        return pltpu.make_async_copy(x_hbm.at[at], xs.at[me, at], ld.at[n])

    def own(n):
        at = pl.ds((1 - core if n == 0 else core) * hu, hu)
        return send(x_hbm.at[at], xs.at[me, at], xs_s.at[0], own_r.at[n], mate)

    def gather(p):
        blk, at, n, m = ((0, 0, 1, 0), (0, 1, hu // 2 - 1, 0), (0, hu // 2, hu // 2, 1), (1, 0, 1, 2), (1, 1, hu // 2 - 1, 2), (1, hu // 2, hu // 2, 3))[p]
        at = xs.at[base + blk, pl.ds(core * hu + at, n)]
        return send(at, at, xs_s.at[0], ag_r.at[m], peer)

    def quarter(m):
        return xs.at[far + m // 2, pl.ds(core * hu + m % 2 * (hu // 2), hu // 2)]

    def relay(m):
        return send(quarter(m), quarter(m), xs_s.at[0], rl_r.at[m // 2], mate)

    def relays(ms):
        for m in ms:
            all_of(quarter(m), ag_r.at[m]).wait()
            relay(m).start()

    def weights_q(n):
        return pltpu.make_async_copy(wq_hbm.at[:, pl.ds(pl.multiple_of(n * TILE, TILE), TILE)], wq.at[n], ld.at[5])

    def weights_o(n):
        return pltpu.make_async_copy(wo_hbm.at[:, pl.ds(pl.multiple_of(n * TILE, TILE), TILE)], wo.at[n], wo_ld)

    wide = kv * HEAD
    small = [
        pltpu.make_async_copy(gain_hbm, gain, ld.at[3]),
        pltpu.make_async_copy(tab_hbm, tab, ld.at[0]),
        pltpu.make_async_copy(wk_hbm, wkv.at[:, pl.ds(0, wide)], ld.at[4]),
        pltpu.make_async_copy(wv_hbm, wkv.at[:, pl.ds(wide, wide)], ld.at[4]),
    ]

    def norm(blk):
        step = 32
        units = step // xs.shape[2]

        def some(i, _):
            at = (blk, pl.ds(i * units, units))
            total = jnp.zeros((step, 128), F32)
            for c in range(0, d, 128):
                w = xs[(*at, slice(None), pl.ds(c, 128))].reshape(step, 128).astype(F32)
                total = total + w * w
            scale = lax.rsqrt(jnp.sum(total, axis=1, keepdims=True) * (1 / d) + 1e-6)
            for c in range(0, d, 128):
                w = xs[(*at, slice(None), pl.ds(c, 128))].reshape(step, 128).astype(F32)
                a[pl.ds(pl.multiple_of(i * step, step), step), pl.ds(c, 128)] = (w * scale * gain_w[pl.ds(c // 128, 1), :]).astype(BF16)
            return 0

        lax.fori_loop(0, rows // step, some, 0)

    def turned(t):
        t = t.astype(BF16).astype(F32)
        return (t * rope[0] + pltpu.roll(t, HEAD // 2, 1) * rope[1]).astype(BF16)

    def project(blk, loading):
        t = tab[pl.ds(pl.multiple_of(blk * rows, rows), rows), :]
        r = pltpu.roll(t, HEAD // 2, 1)
        first = lax.broadcasted_iota(jnp.int32, t.shape, 1) < HEAD // 2
        rope[0] = jnp.where(first, t, r)
        rope[1] = jnp.where(first, -r, t)
        if loading:
            all_of(wkv, ld.at[4]).wait()
        got = _dot(a[...], wkv[...])
        for i in range(kv):
            k[blk, i] = turned(got[:, i * HEAD : (i + 1) * HEAD])
            vt[blk, i, :HEAD, :] = got[:, wide + i * HEAD : wide + (i + 1) * HEAD].T.astype(BF16)

        if loading:
            all_of(wq, ld.at[5]).wait()

        def some(n, _):
            got = _dot(a[...], wq[n])
            for i in range(TILE // HEAD):
                q[blk, n * (TILE // HEAD) + i] = turned(got[:, i * HEAD : (i + 1) * HEAD])
            return 0

        lax.fori_loop(0, nq, some, 0)

    def attend(blk):
        e = HEAD**-0.5 * LOG2E
        deep = vt.shape[2]
        pieces = [(i, i * group + n) for i in range(kv) for n in range(0, group, per)]
        top[...] = jnp.full(top.shape, LOWEST, F32)
        mix[...] = jnp.zeros(mix.shape, F32)

        def block(j, masked):
            scores = [_dot(k[j, i], q[blk, pl.ds(n, per)].reshape(STRIP, HEAD), 1, 1) for i, n in pieces]
            weights, keeps = [], []
            for p, s in enumerate(scores):
                if masked:
                    s = jnp.where(gap[...] >= 0, s, LOWEST)
                old = top[p : p + 1, :]
                new = jnp.maximum(old, s.max(axis=0, keepdims=True))
                top[p : p + 1, :] = new
                weights.append(jnp.exp2((s - new) * e).astype(BF16))
                keeps.append(jnp.exp2((old - new) * e))
            for p, (w, keep) in enumerate(zip(weights, keeps)):
                at = pl.ds(p * deep, deep)
                mix[at, :] = mix[at, :] * keep + _dot(vt[j, pieces[p][0]], w)

        lax.fori_loop(0, blk, lambda j, _: (block(j, False), 0)[1], 0)
        block(blk, True)
        for p, (i, n) in enumerate(pieces):
            got = mix[p * deep : p * deep + HEAD, :] * (1 / mix[p * deep + HEAD : p * deep + HEAD + 1, :])
            for m in range(per):
                seen[:, (n + m) * HEAD : (n + m + 1) * HEAD] = got[:, m * rows : (m + 1) * rows].T.astype(BF16)

    def out_part(n):
        return _dot(seen[...], wo[n])

    def pass_on(b, t):
        return send(pp_out.at[t], pp_in.at[b * half + t], pp_s, pp_r.at[t], mate)

    def scatter(b, t):
        return send(rs_out.at[b * half + t], rs_in.at[t, core], rs_s[b], rs_r.at[t // (half - 1)], far + b)

    def give(b):
        def mates(t):
            pp_out[t] = out_part((1 - core) * half + t).astype(BF16)
            pass_on(b, t).start()

        def mine(t):
            got = out_part(core * half + t)
            pass_on(b, t).wait_recv()
            rs_out[b * half + t] = (got + pp_in[b * half + t].astype(F32)).astype(BF16)
            scatter(b, t).start()

        def both(t, _):
            mates(t + 1)
            mine(t)
            return 0

        if b:
            all_of(pp_out, pp_s).wait()
        mates(0)
        lax.fori_loop(0, half - 1, both, 0)
        mine(half - 1)

    def last(n):
        return send(fin_out(n), fin_in.at[n], fin_s, fin_r, mate)

    def place(i):
        return (i % 2) * half + i // 2

    def mates_rows(i, _):
        n = place(i)
        fin_out(n)[...] = out_part(n).astype(BF16)
        last(n).start()
        return 0

    def my_rows(t, _):
        for h in range(2):
            n = h * half + t
            got = out_part(n)
            mine = xs[me, :, :, pl.ds(pl.multiple_of(n * TILE, TILE), TILE)].reshape(rows, TILE).astype(F32)
            mix[h * rows : (h + 1) * rows, :] = mine + (got + fin_in[n].astype(F32))
        @pl.when(t == 0)
        def _():
            all_of(rs_in.at[pl.ds(0, half - 1)], rs_r.at[0]).wait()

        @pl.when(t == half - 1)
        def _():
            all_of(rs_in.at[half - 1], rs_r.at[1]).wait()

        for h in range(2):
            at = pl.ds(pl.multiple_of((h * half + t) * TILE, TILE), TILE)
            y[:, at] = (mix[h * rows : (h + 1) * rows, :] + rs_in[t, h].astype(F32)).astype(BF16)
        return 0

    barrier = pltpu.get_barrier_semaphore()
    for to in (peer, (mate + 2) % 4, mate):
        pl.semaphore_signal(barrier, 1, device_id={"tp": to}, device_id_type=pl.DeviceIdType.MESH)
    for n in range(3):
        local_x(n).start()
    pl.semaphore_wait(barrier, 3)
    first = pl.ds(core * hu, 1)
    send(x_hbm.at[first], xs.at[me, first], xs_s.at[0], ag_r.at[2 * core], peer).start()
    own(0).start()
    own(1).start()
    local_x(0).wait()
    for copy in small:
        copy.start()
    for n in range(nq):
        weights_q(n).start()
    local_x(1).wait()

    @pl.when(core == 0)
    def _():
        gather(1).start()
        gather(2).start()

    gap[...] = lax.rem(lax.broadcasted_iota(jnp.int32, gap.shape, 1), rows) - lax.broadcasted_iota(jnp.int32, gap.shape, 0)
    vt[:, :, HEAD:, :] = jnp.ones((4, kv, vt.shape[2] - HEAD, rows), BF16)

    local_x(2).wait()
    small[0].wait()
    gain_w[...] = gain[...].astype(F32)
    norm(me)

    own(0).wait_recv()

    @pl.when(core == 0)
    def _():
        gather(3).start()

    @pl.when(core == 1)
    def _():
        for p in range(3):
            gather(p).start()

    gather(4).start()
    gather(5).start()

    small[1].wait()
    project(me, True)
    for n in range(no):
        weights_o(n).start()
    own(1).wait_recv()
    norm(mate)
    project(mate, False)

    for b in range(2):
        relays(((0, 1), (3,))[b])
        all_of(xs.at[far + b, pl.ds((1 - core) * hu, hu)], rl_r.at[b]).wait()
        norm(far + b)
        project(far + b, False)
        attend(far + b)
        if b == 0:
            relays((2,))
            all_of(wo, wo_ld).wait()
        give(b)

    attend(mate)
    lax.fori_loop(0, no, mates_rows, 0)
    attend(me)

    all_of(xs.at[pl.ds(0, 3)], xs_s.at[0]).wait()
    all_of(pp_out, pp_s).wait()
    all_of(fin_in, fin_s).wait()
    all_of(pp_out, rs_s[0]).wait()
    all_of(fin_in, fin_r).wait()

    lax.fori_loop(0, half, my_rows, 0)

    all_of(pp_out, rs_s[1]).wait()


def _table(tokens):
    half = HEAD // 2
    angle = np.arange(tokens, dtype=np.float32)[:, None] * np.float32(THETA) ** (-np.arange(half, dtype=np.float32) / np.float32(half))
    angle = angle.astype(np.float64)
    return np.concatenate([np.cos(angle), np.sin(angle)], -1).astype(np.float32)


def solution(mesh):
    def step(x, gain, wq, wk, wv, wo):
        rows, d = x.shape
        heads, kv = wq.shape[1] // HEAD, wk.shape[1] // HEAD
        nq, no = wq.shape[1] // TILE, d // TILE
        strips = heads * rows // STRIP
        dma = lambda n: pltpu.SemaphoreType.DMA((n,))
        vm = pltpu.VMEM
        tokens = 4 * rows
        return pl.pallas_call(
            _layer,
            out_shape=pltpu.VMEM((rows, d), BF16),
            in_specs=[pl.BlockSpec(memory_space=pl.ANY)] * 7,
            out_specs=pl.BlockSpec(memory_space=pltpu.VMEM),
            scratch_shapes=[
                vm((nq, d, TILE), BF16), vm((d, 2 * kv * HEAD), BF16), vm((no, heads * HEAD, TILE), BF16),
                vm((4, rows // 16, 16, d), BF16), vm((rows, d), BF16), vm((d // 128, 128), BF16), vm((d // 128, 128), F32), vm((tokens, HEAD), F32), vm((2, rows, HEAD), F32),
                vm((4, heads, rows, HEAD), BF16), vm((4, kv, rows, HEAD), BF16), vm((4, kv, HEAD + 16, rows), BF16),
                vm((strips, STRIP), F32), vm((strips * (HEAD + 16), STRIP), F32), vm((rows, STRIP), jnp.int32), vm((rows, heads * HEAD), BF16),
                vm((no // 2, rows, TILE), BF16), vm((no, rows, TILE), BF16), vm((no, rows, TILE), BF16), vm((no // 2, 2, rows, TILE), BF16),
                vm((no, rows, TILE), BF16),
                dma(6), dma(2), dma(1), dma(4), dma(2), dma(no // 2), dma(2),
            ],
            compiler_params=pltpu.CompilerParams(collective_id=0, has_side_effects=True, vmem_limit_bytes=247 * 2**18),
            cost_estimate=pl.CostEstimate(flops=33 * 10**9, bytes_accessed=34 * 2**20, transcendentals=8 * 2**20),
            name="layer",
        )(x.reshape(rows // 16, 16, d), gain.reshape(d // 128, 128), jnp.asarray(_table(tokens)), wq, wk, wv, wo)

    tokens, columns = P(("dp", "tp"), None), P(None, "tp")
    return jax.shard_map(
        step,
        mesh=mesh,
        in_specs=(tokens, P(None), columns, columns, columns, P("tp", None)),
        out_specs=tokens,
        check_vma=False,
    )
```
